256 devices in a mesh: gx: 4 (over x_lo, core), gy: 8 (over z), gz: 8 (over x_hi, y).
Axes of the slice: x: 4 (x_hi: 2, x_lo: 2; x = x_hi * 2 + x_lo), y: 4, z: 8, core: 2. Of those that a mesh axis runs over, the one named last changes fastest.
Arguments:
- fractions: float32 [4, 8, 8, 3, 256], P('gx', 'gy', 'gz'), may hold values from 0 to 1
- velocity: float32 [4, 8, 8, 3, 256], P('gx', 'gy', 'gz'), may hold values from -30 to 30
- charge: float32 [4, 8, 8, 256], P('gx', 'gy', 'gz'), may hold values from -1.5 to 1.5
- drude_charge: float32 [4, 8, 8, 256], P('gx', 'gy', 'gz'), may hold values from -2.2 to -0.8
- screening: float32 [4, 8, 8, 256], P('gx', 'gy', 'gz'), may hold values from 0.2 to 2
- labels: int32 [4, 8, 8, 256], P('gx', 'gy', 'gz'), may hold values from 0 to 255
- masses: float32 [4, 8, 8, 256], P('gx', 'gy', 'gz'), may hold values from 4 to 32
- counts: int32 [4, 8, 8], P('gx', 'gy', 'gz'), may hold values from 128 to 256, as said below
- leaving: int32 [4, 8, 8, 6, 16], P('gx', 'gy', 'gz'), may hold values from -1 to 255, as said below
Outputs:
- staying: float32 [4, 8, 8, 9, 256], P('gx', 'gy', 'gz')
- arrivals: float32 [4, 8, 8, 14, 96], P('gx', 'gy', 'gz')
The draws below stay inside these ranges and needn't reach their ends.
Inputs may be any that keep to these rules, and one draw needn't show every extreme that they name: `counts`: at least one box holds 256 atoms. `leaving`: entries name distinct live slots of their box, or are -1; in every box some face has all 16 entries used.
All inputs are finite; a program needn't handle non-finite values.
Results may differ from the reference program's by a relative error of at most 0.0003.
Values sent between devices are 32-bit elements; how exact they have to be, the bound alone decides.
A program may use at most 64 MiB of HBM per device.

```python
import math
import jax
import jax.numpy as jnp
from jax import lax

SLOTS = 256
MOVE = 16
ITERS = 3
BX = 4
BY = 8
BZ = 8


def lattice_size():
    lattice = 1
    while lattice * lattice * lattice < SLOTS:
        lattice = lattice + 1
    return lattice


def draw_fractions(key, part):
    lattice = lattice_size()
    box_total = BX * BY * BZ
    subkeys = jax.random.split(jax.random.fold_in(key, 3), box_total)
    chosen = jax.vmap(lambda subkey: jax.random.permutation(subkey, lattice * lattice * lattice)[:SLOTS])(subkeys)
    cell_ids = jnp.stack([chosen // (lattice * lattice), chosen // lattice % lattice, chosen % lattice], axis=1)
    jitters = jax.random.uniform(jax.random.fold_in(key, 5), (box_total, 3, SLOTS), jnp.float32, -0.3, 0.3)
    values = (cell_ids.astype(jnp.float32) + 0.5 + jitters) / lattice
    return values.reshape((BX, BY, BZ, 3, SLOTS))


def box_counts(key):
    box_total = BX * BY * BZ
    root_key = jax.random.fold_in(key, 17)
    sampled = jax.random.randint(jax.random.fold_in(root_key, 1), (box_total,), SLOTS // 2, SLOTS + 1)
    fullest = jax.random.randint(jax.random.fold_in(root_key, 2), (), 0, box_total)
    return jnp.where(jnp.arange(box_total) == fullest, SLOTS, sampled).astype(jnp.int32)


def draw_counts(key, part):
    return box_counts(key).reshape((BX, BY, BZ))


def draw_leaving(key, part):
    box_total = BX * BY * BZ
    box_sizes = box_counts(key)
    root_key = jax.random.fold_in(key, 29)

    def one_box(subkey, box_count):
        shuffled = jax.random.permutation(subkey, SLOTS)
        ranked = shuffled[jnp.argsort(jnp.where(shuffled < box_count, 0, 1), stable=True)]
        return ranked[:6 * MOVE].reshape((6, MOVE))
    chosen = jax.vmap(one_box)(jax.random.split(jax.random.fold_in(root_key, 1), box_total), box_sizes)
    lengths = jax.random.randint(jax.random.fold_in(root_key, 2), (box_total, 6), MOVE // 3, MOVE + 1)
    fullest = jax.random.randint(jax.random.fold_in(root_key, 3), (box_total,), 0, 6)
    lengths = jnp.where(lax.broadcasted_iota(jnp.int32, (box_total, 6), 1) == fullest[:, None], MOVE, lengths)
    occupied = lax.broadcasted_iota(jnp.int32, (box_total, 6, MOVE), 2) < lengths[:, :, None]
    return jnp.where(occupied, chosen, -1).reshape((BX, BY, BZ, 6, MOVE)).astype(jnp.int32)


def plant(entries, stream_key, low, largest):
    longest = entries.shape.index(max(entries.shape))
    spots = []
    for shift in (0, 1):
        where = [jax.random.randint(jax.random.fold_in(stream_key, axis), (), 0, length) for axis, length in enumerate(entries.shape)]
        where[longest] = (where[longest] + shift) % entries.shape[longest]
        spots.append(tuple(where))
    return entries.at[spots[0]].set(low).at[spots[1]].set(largest)


def levels(key, shape, shards, low, largest):
    factor_of, own = 1.0, jax.random.fold_in(key, 6)
    for axis_at, parts in shards:
        draws = jnp.exp(jax.random.uniform(jax.random.fold_in(own, axis_at), (parts,), jnp.float32, low / len(shards), largest / len(shards)))
        factor_of = factor_of * jnp.repeat(draws, shape[axis_at] // parts).reshape([-1 if axis == axis_at else 1 for axis in range(len(shape))])
    return factor_of


def scatter_about(stream_key, extent, spread, reach, cuts=(), kind=jnp.bfloat16):
    entries = jax.random.normal(stream_key, extent, jnp.float32) * spread
    if len(cuts) > 0:
        entries = levels(stream_key, extent, cuts, -0.22, 0.18) * entries
    return jnp.clip(entries, min=-reach, max=reach).astype(kind)


def setup_inputs(seed: int = 0) -> dict:
    arg_keys = jax.random.split(jax.random.key(seed), 10)
    return {
        "fractions": draw_fractions(jax.random.fold_in(arg_keys[9], 71), 0),
        "velocity": scatter_about(arg_keys[1], (BX, BY, BZ, 3, SLOTS), 5.0, 30.0, ((0, 4), (1, 8), (2, 8)), jnp.float32),
        "charge": scatter_about(arg_keys[2], (BX, BY, BZ, SLOTS), 0.5, 1.5, ((0, 4), (1, 8), (2, 8)), jnp.float32),
        "drude_charge": jnp.clip(-2.2 + 1.40000004 * jax.random.uniform(arg_keys[3], (BX, BY, BZ, SLOTS), jnp.float32) ** levels(arg_keys[3], (BX, BY, BZ, SLOTS), ((0, 4), (1, 8), (2, 8)), -0.2, 0.2), -2.2, -0.8),
        "screening": jnp.clip(jnp.exp(math.log(2.0) - 2.3025851 * jax.random.uniform(arg_keys[4], (BX, BY, BZ, SLOTS), jnp.float32) ** levels(arg_keys[4], (BX, BY, BZ, SLOTS), ((0, 4), (1, 8), (2, 8)), -0.2, 0.2)), 0.2, 2.0),
        "labels": plant(jax.random.randint(arg_keys[5], (BX, BY, BZ, SLOTS), 0, SLOTS), jax.random.fold_in(arg_keys[5], 1), 0, SLOTS - 1).astype(jnp.int32),
        "masses": jnp.clip(jnp.exp(math.log(32.0) - 2.0794415 * jax.random.uniform(arg_keys[6], (BX, BY, BZ, SLOTS), jnp.float32) ** levels(arg_keys[6], (BX, BY, BZ, SLOTS), ((0, 4), (1, 8), (2, 8)), -0.2, 0.2)), 4.0, 32.0),
        "counts": draw_counts(jax.random.fold_in(arg_keys[9], 71), 0),
        "leaving": draw_leaving(jax.random.fold_in(arg_keys[9], 71), 0),
    }


CUTOFF = 12.0
DRUDE_GAIN = 0.3320636
KICK = 0.002 * 418.4 * 332.0636
TIMESTEP = 0.002
UNITS = ((1, 0, 0), (-1, 0, 0), (0, 1, 0), (0, -1, 0), (0, 0, 1), (0, 0, -1))

def box_length():
    return max(12.0, (10.0 * SLOTS) ** (1.0 / 3.0))

def block_terms(target, source, moments, offset, same_box, charges, dipoles):
    length = box_length()
    slot_count = target.shape[-1]
    deltas = [(target[dimension][:, None] - source[dimension][None, :] - offset[dimension]) * length for dimension in range(3)]
    dist_sq = deltas[0] * deltas[0] + deltas[1] * deltas[1] + deltas[2] * deltas[2]
    row_ids = lax.broadcasted_iota(jnp.int32, (slot_count, slot_count), 0)
    col_ids = lax.broadcasted_iota(jnp.int32, (slot_count, slot_count), 1)
    itself = jnp.logical_and(same_box, row_ids == col_ids)
    dist_sq = jnp.where(itself, 1.0, dist_sq)
    inside = jnp.logical_and(dist_sq < CUTOFF * CUTOFF, jnp.logical_not(itself))
    switch = jnp.where(inside, jnp.square(1.0 - dist_sq / (CUTOFF * CUTOFF)), 0.0)
    inverse = lax.rsqrt(dist_sq)
    radial = switch * inverse * inverse * inverse
    alpha_target = DRUDE_GAIN * target[4] * target[4]
    alpha_source = DRUDE_GAIN * source[4] * source[4]
    damping = 0.5 * (target[5][:, None] + source[5][None, :]) * lax.rsqrt(alpha_target[:, None] * alpha_source[None, :])
    exponent = damping * dist_sq * jnp.sqrt(dist_sq)
    screen_three = -jnp.expm1(-exponent)
    screen_five = screen_three - exponent * jnp.exp(-exponent)
    fields = [jnp.zeros((slot_count,), target.dtype) for dimension in range(3)]
    if charges:
        allowed = target[6][:, None] != source[6][None, :]
        weight = jnp.where(allowed, radial * screen_three * source[3][None, :], 0.0)
        fields = [fields[dimension] + lax.optimization_barrier(jnp.sum(weight * deltas[dimension], axis=1)) for dimension in range(3)]
    if dipoles:
        moment = [source[4] * moments[dimension] for dimension in range(3)]
        projected = deltas[0] * moment[0][None, :] + deltas[1] * moment[1][None, :] + deltas[2] * moment[2][None, :]
        dipolar = 3.0 * radial * screen_five * inverse * inverse * projected
        direct = radial * screen_three
        fields = [fields[dimension] + lax.optimization_barrier(jnp.sum(dipolar * deltas[dimension] - direct * moment[dimension][None, :], axis=1)) for dimension in range(3)]
    return jnp.stack(fields)

def grid_field(statics, moments, charges, dipoles):
    box_total = statics.shape[0] * statics.shape[1] * statics.shape[2]
    group_size = math.gcd(box_total, 8)
    layout = (box_total // group_size, group_size)
    targets = statics.reshape(layout + statics.shape[3:])
    summed = jnp.zeros(statics.shape[:3] + (3, statics.shape[-1]), statics.dtype)
    for shift_x in (-1, 0, 1):
        for shift_y in (-1, 0, 1):
            for shift_z in (-1, 0, 1):
                rolled = (-shift_x, -shift_y, -shift_z)
                sources = jnp.roll(statics, rolled, axis=(0, 1, 2)).reshape(layout + statics.shape[3:])
                source_moments = jnp.roll(moments, rolled, axis=(0, 1, 2)).reshape(layout + moments.shape[3:])
                offset = (float(shift_x), float(shift_y), float(shift_z))
                same_box = shift_x == 0 and shift_y == 0 and (shift_z == 0)

                def per_group(arrays, offset=offset, same_box=same_box):

                    def single(target_row, source_row, moment_row):
                        return block_terms(target_row, source_row, moment_row, offset, same_box, charges, dipoles)
                    return jax.vmap(single)(arrays[0], arrays[1], arrays[2])
                blocks = lax.map(per_group, (targets, sources, source_moments))
                summed = summed + blocks.reshape(summed.shape)
    return summed

def reference(fractions, velocity, charge, drude_charge, screening, labels, masses, counts, leaving):
    slot_ids = lax.broadcasted_iota(jnp.int32, charge.shape, 3)
    is_live = slot_ids < counts[..., None]
    charge_live = jnp.where(is_live, charge, 0.0)
    drude_live = jnp.where(is_live, drude_charge, -1.0)
    label_values = labels.astype(fractions.dtype)
    statics = jnp.concatenate([fractions, charge_live[..., None, :], drude_live[..., None, :], screening[..., None, :], label_values[..., None, :]], axis=3)
    permanent = grid_field(statics, statics[:, :, :, :3], True, False)
    fields = permanent
    shifts = jnp.zeros_like(fractions)
    for iteration in range(ITERS):
        shifts = jnp.where(is_live[..., None, :], DRUDE_GAIN * drude_live[..., None, :] * fields, 0.0)
        fields = permanent + grid_field(statics, shifts, False, True)
    velocity_new = velocity + KICK * charge_live[..., None, :] * fields / masses[..., None, :]
    fractions_new = fractions + TIMESTEP * velocity_new / box_length()
    members = leaving[..., None] == lax.broadcasted_iota(jnp.int32, leaving.shape + (SLOTS,), 5)
    departed = jnp.any(members, axis=(3, 4))
    remain = jnp.logical_and(is_live, jnp.logical_not(departed))
    staying = jnp.where(remain[..., None, :], jnp.concatenate([fractions_new, velocity_new, shifts], axis=3), 0.0)
    complete = jnp.concatenate([fractions_new, velocity_new, shifts, charge_live[..., None, :], drude_live[..., None, :], screening[..., None, :], label_values[..., None, :], masses[..., None, :]], axis=3)
    pieces = []
    for direction in range(6):
        heading = UNITS[direction]
        sources = jnp.roll(complete, heading, axis=(0, 1, 2))
        slot_lists = jnp.roll(leaving[:, :, :, direction, :], heading, axis=(0, 1, 2))
        present = slot_lists >= 0
        indices = jnp.broadcast_to(jnp.maximum(slot_lists, 0)[..., None, :], sources.shape[:3] + (14, slot_lists.shape[-1]))
        picked = jnp.take_along_axis(sources, indices, axis=4)
        picked = jnp.where(present[..., None, :], picked, 0.0)
        frame_moves = jnp.zeros((14,), picked.dtype).at[0:3].set(-jnp.array(heading, picked.dtype))
        picked = picked + frame_moves[:, None] * present[..., None, :].astype(picked.dtype)
        pieces.append(picked)
    arrivals = jnp.concatenate(pieces, axis=4)
    return (staying, arrivals)
```

```python
import functools
import math

import jax
import jax.numpy as jnp
from jax import lax
from jax.experimental import pallas as pl
from jax.experimental.pallas import tpu as pltpu
from jax.sharding import PartitionSpec as P

SLOTS = 256
MOVE = 16
ITERS = 3
CUTOFF = 12.0
DRUDE_GAIN = 0.3320636
KICK = 0.002 * 418.4 * 332.0636
TIMESTEP = 0.002
UNITS = ((1, 0, 0), (-1, 0, 0), (0, 1, 0), (0, -1, 0), (0, 0, 1), (0, 0, -1))
EDGE = max(12.0, (10.0 * SLOTS) ** (1.0 / 3.0))
SCALE = EDGE / CUTOFF
LN2 = math.log(2.0)
GROUPS = SLOTS // 8
CHUNK = 4
AXES = ("gx", "gy", "gz")
MESH = pl.DeviceIdType.MESH
HIGHEST = lax.Precision.HIGHEST


def code_offset(code):
    return lax.rem(code + 1, 3) - 1 if not isinstance(code, int) else (code + 1) % 3 - 1


def step_from(mine, sizes, step):
    return tuple(lax.rem(mine[a] + step[a] + sizes[a], sizes[a]) for a in range(3))


def columns(row):
    return jnp.transpose(jnp.broadcast_to(row, (128, SLOTS))).reshape(GROUPS, 8, 128)


def lane_sums(block):
    return jnp.sum(jnp.transpose(block.reshape(SLOTS, 128)), axis=0, keepdims=True)


def kernel(
    sizes,
    counts_ref,
    fractions_ref,
    velocity_ref,
    charge_ref,
    drude_ref,
    screening_ref,
    labels_ref,
    masses_ref,
    leaving_ref,
    staying_ref,
    arrivals_ref,
    statics,
    places,
    moments,
    target,
    coef_a,
    coef_b,
    totals,
    outbox,
    inbox,
    static_send,
    static_recv,
    moment_send,
    moment_recv,
    out_send,
    out_recv,
):
    mine = tuple(lax.axis_index(axis) for axis in AXES)
    steps = [(code_offset(k % 3), code_offset(k // 3 % 3), code_offset(k // 9)) for k in range(27)]
    peers = [step_from(mine, sizes, step) for step in steps]
    mirror = [(3 - k % 3) % 3 + 3 * ((3 - k // 3 % 3) % 3) + 9 * ((3 - k // 9) % 3) for k in range(27)]

    barrier = pltpu.get_barrier_semaphore()
    for k in range(26, 0, -1):
        pl.semaphore_signal(barrier, inc=1, device_id=peers[k], device_id_type=MESH)

    count = counts_ref[0, 0, 0]
    slots = lax.broadcasted_iota(jnp.int32, (1, SLOTS), 1)
    live = slots < count
    fractions = fractions_ref[0, 0, 0]
    charge = jnp.where(live, charge_ref[0, 0], 0.0)
    drude = jnp.where(live, drude_ref[0, 0], -1.0)
    screening = screening_ref[0, 0]
    label = labels_ref[0, 0].astype(jnp.float32)
    place = (fractions - 0.5) * SCALE
    root = math.sqrt(0.5 * CUTOFF**3 / LN2) * lax.rsqrt(DRUDE_GAIN * drude * drude)
    statics[0, 0:3] = place
    statics[0, 3:4] = charge * (1.0 / CUTOFF**2)
    statics[0, 4:5] = root
    statics[0, 5:6] = screening
    statics[0, 6:7] = label
    statics[0, 7:8] = jnp.zeros((1, SLOTS), jnp.float32)
    places[0, 0:3] = place
    for at, row in enumerate((place[0:1], place[1:2], place[2:3], -root, screening, label)):
        target[at] = columns(row)

    pl.semaphore_wait(barrier, 26)

    def static_copy(k, slot, device):
        return pltpu.make_async_remote_copy(
            src_ref=statics.at[0],
            dst_ref=statics.at[slot],
            send_sem=static_send.at[k],
            recv_sem=static_recv.at[slot],
            device_id=device,
            device_id_type=MESH,
        )

    def moment_copy(turn, k, slot, device):
        return pltpu.make_async_remote_copy(
            src_ref=moments.at[turn, 0],
            dst_ref=moments.at[turn, slot],
            send_sem=moment_send.at[turn, k],
            recv_sem=moment_recv.at[turn, slot],
            device_id=device,
            device_id_type=MESH,
        )

    for k in range(26, 0, -1):
        static_copy(k, mirror[k], peers[k]).start()

    def spread(row):
        return jnp.broadcast_to(row, (8, 128))

    def geometry(k, own):
        for half in range(2):
            lanes = pl.ds(half * 128, 128)
            source = [spread(places[k, d : d + 1, lanes]) for d in range(3)]
            source += [spread(statics[k, d : d + 1, lanes]) for d in range(3, 7)]

            def chunk(c, carry, half=half, lanes=lanes, source=source):
                at = pl.ds(c * CHUNK, CHUNK)
                deltas = [target[d, at] - source[d] for d in range(3)]
                dist_sq = deltas[0] * deltas[0] + deltas[1] * deltas[1] + deltas[2] * deltas[2]
                if own:
                    rows = c * (CHUNK * 8) + lax.broadcasted_iota(jnp.int32, (CHUNK, 8, 128), 0) * 8
                    rows = rows + lax.broadcasted_iota(jnp.int32, (CHUNK, 8, 128), 1)
                    cols = lax.broadcasted_iota(jnp.int32, (CHUNK, 8, 128), 2) + half * 128
                    dist_sq = jnp.where(rows == cols, 1.0, dist_sq)
                inverse = lax.rsqrt(dist_sq)
                inside = jnp.maximum(1.0 - dist_sq, 0.0)
                inverse_sq = inverse * inverse
                radial = (inside * inside) * inverse * inverse_sq
                cubed = dist_sq * dist_sq * inverse
                power = (target[4, at] + source[5]) * (target[3, at] * source[4]) * cubed
                decay = jnp.exp2(power)
                three = 1.0 - decay
                five = three + (power * LN2) * decay
                direct = radial * three
                coef_b[k, at, :, lanes] = direct
                coef_a[k, at, :, lanes] = (radial * 3.0) * inverse_sq * five
                weight = jnp.where(target[5, at] != source[6], direct * source[3], 0.0)
                for d in range(3):
                    if own and half == 0:
                        totals[d, at] = weight * deltas[d]
                    else:
                        totals[d, at] += weight * deltas[d]
                return carry

            lax.fori_loop(0, GROUPS // CHUNK, chunk, 0, unroll=True)

    geometry(0, True)

    def static_box(k, carry):
        static_copy(k, k, mine).wait_recv()
        for d, step in enumerate((lax.rem(k, 3), lax.rem(k // 3, 3), k // 9)):
            moved = code_offset(step).astype(jnp.float32) * SCALE
            places[k, d : d + 1] = statics[k, d : d + 1] + moved
        geometry(k, False)
        return carry

    lax.fori_loop(1, 27, static_box, 0)

    permanent = [lane_sums(totals[d]) for d in range(3)]
    permanent = jnp.concatenate(permanent, axis=0)
    to_shift = jnp.where(live, DRUDE_GAIN * drude, 0.0)
    to_moment = to_shift * drude * (1.0 / CUTOFF**3)

    def induced(turn, k):
        mu = [moments[turn, k, d : d + 1] for d in range(3)]
        xs = [places[k, d : d + 1] for d in range(3)]
        along = xs[0] * mu[0] + xs[1] * mu[1] + xs[2] * mu[2]
        for half in range(2):
            lanes = pl.ds(half * 128, 128)
            sl = slice(half * 128, half * 128 + 128)
            m = [spread(moments[turn, k, d : d + 1, lanes]) for d in range(3)]
            x = [spread(places[k, d : d + 1, lanes]) for d in range(3)]
            s = spread(along[:, sl])

            def chunk(c, carry, lanes=lanes, m=m, x=x, s=s):
                at = pl.ds(c * CHUNK, CHUNK)
                proj = target[0, at] * m[0] + target[1, at] * m[1] + target[2, at] * m[2] - s
                dipolar = coef_a[k, at, :, lanes] * proj
                direct = coef_b[k, at, :, lanes]
                totals[3, at] += dipolar
                for d in range(3):
                    totals[d, at] += dipolar * x[d] + direct * m[d]
                return carry

            lax.fori_loop(0, GROUPS // CHUNK, chunk, 0, unroll=True)

    def turn_body(turn, fields):
        moments[turn, 0] = jnp.concatenate([to_moment * fields, jnp.zeros((1, SLOTS), jnp.float32)], axis=0)
        for k in range(26, 0, -1):
            moment_copy(turn, k, mirror[k], peers[k]).start()
        totals[...] = jnp.zeros_like(totals)

        def moment_box(k, carry):
            @pl.when(k > 0)
            def _():
                moment_copy(turn, k, k, mine).wait_recv()

            induced(turn, k)
            return carry

        lax.fori_loop(0, 27, moment_box, 0)
        plain = lane_sums(totals[3])
        rows = [place[d : d + 1] * plain - lane_sums(totals[d]) for d in range(3)]
        return permanent + jnp.concatenate(rows, axis=0)

    before = lax.fori_loop(0, ITERS - 1, turn_body, permanent)
    fields = turn_body(ITERS - 1, before)
    shifts = to_shift * before

    def drain(k, carry):
        static_copy(k, k, mine).wait_send()
        for turn in range(ITERS):
            moment_copy(turn, k, k, mine).wait_send()
        return carry

    velocity = velocity_ref[0, 0, 0] + KICK * charge * fields / masses_ref[0, 0]
    moved = fractions + (TIMESTEP / EDGE) * velocity

    lists = leaving_ref[0, 0, 0].astype(jnp.float32)
    lane = lax.broadcasted_iota(jnp.int32, (MOVE, 128), 1)
    pick = jnp.where(lax.rem(lane, MOVE) == lax.broadcasted_iota(jnp.int32, (MOVE, 128), 0), 1.0, 0.0)
    tiled = jnp.dot(lists, pick, precision=HIGHEST, preferred_element_type=jnp.float32)
    lane6 = lax.broadcasted_iota(jnp.int32, (6, 128), 1)
    mine6 = lane6 // MOVE == lax.broadcasted_iota(jnp.int32, (6, 128), 0)
    flat = jnp.sum(jnp.where(mine6, tiled, 0.0), axis=0, keepdims=True)
    lane1 = lax.broadcasted_iota(jnp.int32, (1, 128), 1)
    flat = jnp.where(lane1 < 6 * MOVE, flat, -1.0)
    slot_rows = lax.broadcasted_iota(jnp.int32, (SLOTS, 128), 0).astype(jnp.float32)
    matches = jnp.where(slot_rows == flat, 1.0, 0.0)
    named = lax.dot_general(
        jnp.ones((8, 128), jnp.float32),
        matches,
        (((1,), (1,)), ((), ())),
        preferred_element_type=jnp.float32,
    )[0:1]
    present = jnp.where(flat >= 0.0, 1.0, 0.0)

    complete = jnp.concatenate(
        [
            moved,
            velocity,
            shifts,
            charge,
            drude,
            screening,
            label,
            masses_ref[0, 0],
            jnp.zeros((2, SLOTS), jnp.float32),
        ],
        axis=0,
    )
    packed = jnp.dot(complete, matches, precision=HIGHEST, preferred_element_type=jnp.float32)
    face = lane1 // MOVE
    headings = []
    for d in range(3):
        heading = jnp.where(face == 2 * d, -1.0, 0.0) + jnp.where(face == 2 * d + 1, 1.0, 0.0)
        headings.append(heading * present)
    headings.append(jnp.zeros((13, 128), jnp.float32))
    outbox[...] = packed + jnp.concatenate(headings, axis=0)

    def out_copy(face, device):
        return pltpu.make_async_remote_copy(
            src_ref=outbox,
            dst_ref=inbox.at[face],
            send_sem=out_send.at[face],
            recv_sem=out_recv.at[face],
            device_id=device,
            device_id_type=MESH,
        )

    for at in range(5, -1, -1):
        out_copy(at, step_from(mine, sizes, UNITS[at])).start()
    remain = jnp.logical_and(live, named < 0.5)
    staying_ref[0, 0, 0] = jnp.where(remain, complete[0:9], 0.0)
    lax.fori_loop(1, 27, drain, 0)
    landed = jnp.zeros((16, 128), jnp.float32)
    lane16 = lax.broadcasted_iota(jnp.int32, (16, 128), 1) // MOVE
    for at in range(6):
        out_copy(at, mine).wait_recv()
        landed = jnp.where(lane16 == at, inbox[at], landed)
    arrivals_ref[0, 0, 0] = landed[0:14, 0 : 6 * MOVE]
    for at in range(6):
        out_copy(at, mine).wait_send()


def solution(mesh):
    sizes = tuple(mesh.shape[axis] for axis in AXES)
    vec = P("gx", "gy", "gz", None, None)
    row = P("gx", "gy", "gz", None)
    placed = (vec, vec, row, row, row, row, row, P("gx", "gy", "gz"), vec)
    vmem = pl.BlockSpec(memory_space=pltpu.VMEM)
    smem = pl.BlockSpec(memory_space=pltpu.SMEM)
    call = pl.pallas_call(
        functools.partial(kernel, sizes),
        out_shape=(
            jax.ShapeDtypeStruct((1, 1, 1, 9, SLOTS), jnp.float32),
            jax.ShapeDtypeStruct((1, 1, 1, 14, 6 * MOVE), jnp.float32),
        ),
        in_specs=[smem] + [vmem] * 8,
        out_specs=(vmem, vmem),
        scratch_shapes=[
            pltpu.VMEM((27, 8, SLOTS), jnp.float32),
            pltpu.VMEM((27, 4, SLOTS), jnp.float32),
            pltpu.VMEM((ITERS, 27, 4, SLOTS), jnp.float32),
            pltpu.VMEM((6, GROUPS, 8, 128), jnp.float32),
            pltpu.VMEM((27, GROUPS, 8, SLOTS), jnp.float32),
            pltpu.VMEM((27, GROUPS, 8, SLOTS), jnp.float32),
            pltpu.VMEM((4, GROUPS, 8, 128), jnp.float32),
            pltpu.VMEM((16, 128), jnp.float32),
            pltpu.VMEM((6, 16, 128), jnp.float32),
            pltpu.SemaphoreType.DMA((27,)),
            pltpu.SemaphoreType.DMA((27,)),
            pltpu.SemaphoreType.DMA((ITERS, 27)),
            pltpu.SemaphoreType.DMA((ITERS, 27)),
            pltpu.SemaphoreType.DMA((6,)),
            pltpu.SemaphoreType.DMA((6,)),
        ],
        compiler_params=pltpu.CompilerParams(
            collective_id=0, has_side_effects=True, vmem_limit_bytes=40 * 1024 * 1024
        ),
    )

    def local(fractions, velocity, charge, drude_charge, screening, labels, masses, counts, leaving):
        return call(
            counts, fractions, velocity, charge, drude_charge, screening, labels, masses, leaving
        )

    return jax.shard_map(local, mesh=mesh, in_specs=placed, out_specs=(vec, vec), check_vma=False)
```

```python
import functools
import math

import jax
import jax.numpy as jnp
from jax import lax
from jax.experimental import pallas as pl
from jax.experimental.pallas import tpu as pltpu
from jax.sharding import PartitionSpec as P

SLOTS = 256
MOVE = 16
ITERS = 3
CUTOFF = 12.0
DRUDE_GAIN = 0.3320636
KICK = 0.002 * 418.4 * 332.0636
TIMESTEP = 0.002
UNITS = ((1, 0, 0), (-1, 0, 0), (0, 1, 0), (0, -1, 0), (0, 0, 1), (0, 0, -1))
EDGE = max(12.0, (10.0 * SLOTS) ** (1.0 / 3.0))
SCALE = EDGE / CUTOFF
LN2 = math.log(2.0)
GROUPS = SLOTS // 8
CHUNK = 4
AXES = ("gx", "gy", "gz")
MESH = pl.DeviceIdType.MESH
HIGHEST = lax.Precision.HIGHEST
F32 = jnp.float32
BF16 = jnp.bfloat16


def code_offset(code):
    return (code + 1) % 3 - 1 if isinstance(code, int) else lax.rem(code + 1, 3) - 1


def step_from(mine, sizes, step):
    return tuple(lax.rem(mine[a] + (step[a] + sizes[a]), sizes[a]) for a in range(3))


def columns(row):
    return jnp.transpose(jnp.broadcast_to(row, (128, SLOTS))).reshape(GROUPS, 8, 128)


def split(value):
    high = value.astype(BF16)
    return high, value - high.astype(F32)


def kernel(
    sizes,
    fractions_hbm,
    velocity_hbm,
    charge_hbm,
    drude_hbm,
    screening_hbm,
    labels_hbm,
    masses_hbm,
    counts_hbm,
    leaving_hbm,
    staying_ref,
    arrivals_ref,
    fractions_ref,
    velocity_ref,
    charge_ref,
    drude_ref,
    screening_ref,
    labels_ref,
    masses_ref,
    counts_ref,
    leaving_ref,
    statics,
    places,
    moments,
    even,
    odd,
    coef_a,
    coef_b,
    totals,
    sums_a,
    sums_b,
    chosen,
    latest,
    outbox,
    inbox,
    load_sem,
    static_send,
    static_recv,
    moment_send,
    moment_recv,
    out_send,
    out_recv,
):
    mine = tuple(lax.axis_index(axis) for axis in AXES)
    steps = [(code_offset(k % 3), code_offset(k // 3 % 3), code_offset(k // 9)) for k in range(27)]
    peers = [step_from(mine, sizes, step) for step in steps]
    mirror = [(3 - k % 3) % 3 + 3 * ((3 - k // 3 % 3) % 3) + 9 * ((3 - k // 9) % 3) for k in range(27)]

    barrier = pltpu.get_barrier_semaphore()
    for k in range(26, 0, -1):
        pl.semaphore_signal(barrier, inc=1, device_id=peers[k], device_id_type=MESH)

    pairs = (
        (fractions_hbm, fractions_ref),
        (charge_hbm, charge_ref),
        (drude_hbm, drude_ref),
        (screening_hbm, screening_ref),
        (labels_hbm, labels_ref),
        (counts_hbm, counts_ref),
        (velocity_hbm, velocity_ref),
        (masses_hbm, masses_ref),
        (leaving_hbm, leaving_ref),
    )
    loads = [pltpu.make_async_copy(src, dst, load_sem.at[at]) for at, (src, dst) in enumerate(pairs)]
    for load in loads:
        load.start()
    for load in loads:
        load.wait()

    slots = lax.broadcasted_iota(jnp.int32, (1, SLOTS), 1)
    live = slots < jnp.broadcast_to(counts_ref[0], (1, SLOTS))
    fractions = [fractions_ref[d] for d in range(3)]
    charge = jnp.where(live, charge_ref[0], 0.0)
    drude = jnp.where(live, drude_ref[0], -1.0)
    screening = screening_ref[0]
    label = labels_ref[0].astype(F32)
    place = [(fractions[d] - 0.5) * SCALE for d in range(3)]
    root = math.sqrt(0.5 * CUTOFF**3 / LN2) * lax.rsqrt(DRUDE_GAIN * drude * drude)
    own_rows = place + [root, screening, label, charge * (1.0 / CUTOFF**2)]
    for at, row in enumerate(own_rows):
        statics[0, at : at + 1] = row
    statics[0, 7:8] = jnp.zeros((1, SLOTS), F32)
    for d in range(3):
        places[0, d : d + 1] = place[d]

    pl.semaphore_wait(barrier, 26)

    def static_copy(slot, device):
        return pltpu.make_async_remote_copy(
            src_ref=statics.at[0],
            dst_ref=statics.at[slot],
            send_sem=static_send,
            recv_sem=static_recv.at[(slot - 1) // 2],
            device_id=device,
            device_id_type=MESH,
        )

    def moment_group(slot):
        return 0 if slot < 5 else slot // 9 + (1 if slot < 9 else 1)

    def moment_copy(turn, slot, device):
        return pltpu.make_async_remote_copy(
            src_ref=moments.at[turn, 0],
            dst_ref=moments.at[turn, slot],
            send_sem=moment_send.at[turn],
            recv_sem=moment_recv.at[turn, moment_group(slot)],
            device_id=device,
            device_id_type=MESH,
        )

    def landed(ref, sem):
        pltpu.make_async_copy(ref, ref, sem).wait()

    for k in range(26, 0, -1):
        static_copy(mirror[k], peers[k]).start()

    def fill(k, buffer):
        for at in range(6):
            buffer[at] = columns(places[k, at : at + 1] if at < 3 else statics[k, at : at + 1])
        buffer[6] = columns(statics[k, 6:7])

    def spread(row, half):
        return jnp.broadcast_to(row[:, half * 128 : half * 128 + 128], (8, 128))

    def geometry(k, buffer, own):
        sums = [None] * 6
        for half in range(2):
            goal = [spread(row, half) for row in place + [-root, screening, label]]
            for c in range(GROUPS // CHUNK):
                at = pl.ds(c * CHUNK, CHUNK)
                deltas = [goal[d] - buffer[d, at] for d in range(3)]
                dist_sq = deltas[0] * deltas[0] + deltas[1] * deltas[1] + deltas[2] * deltas[2]
                if own:
                    rows = c * (CHUNK * 8) + lax.broadcasted_iota(jnp.int32, (CHUNK, 8, 128), 0) * 8
                    rows = rows + lax.broadcasted_iota(jnp.int32, (CHUNK, 8, 128), 1)
                    cols = lax.broadcasted_iota(jnp.int32, (CHUNK, 8, 128), 2) + half * 128
                    dist_sq = jnp.where(rows == cols, 1.0, dist_sq)
                inverse = lax.rsqrt(dist_sq)
                inside = jnp.maximum(1.0 - dist_sq, 0.0)
                inverse_sq = inverse * inverse
                radial = (inside * inside) * inverse * inverse_sq
                cubed = dist_sq * dist_sq * inverse
                power = (goal[4] + buffer[4, at]) * (goal[3] * buffer[3, at]) * cubed
                decay = jnp.exp2(power)
                three = 1.0 - decay
                five = three + (power * LN2) * decay
                direct = radial * three
                coef_b[k, at, :, pl.ds(half * 128, 128)] = direct
                coef_a[k, at, :, pl.ds(half * 128, 128)] = radial * inverse_sq * five
                weight = jnp.where(goal[5] != buffer[5, at], direct * buffer[6, at], 0.0)
                for d in range(3):
                    term = jnp.sum(weight * deltas[d], axis=0)
                    old = sums[3 * half + d]
                    sums[3 * half + d] = term if old is None else old + term
        for half in range(2):
            for d in range(3):
                lanes = pl.ds(half * 128, 128)
                if own:
                    totals[d, :, lanes] = sums[3 * half + d]
                else:
                    totals[d, :, lanes] += sums[3 * half + d]

    def arrive(k):
        for d, step in enumerate((lax.rem(k, 3), lax.rem(k // 3, 3), k // 9)):
            moved = code_offset(step).astype(F32) * SCALE
            places[k, d : d + 1] = statics[k, d : d + 1] + moved

    fill(0, even)
    geometry(0, even, True)

    def wait_pair(p):
        landed(statics.at[pl.ds(2 * p + 1, 2)], static_recv.at[p])
        arrive(2 * p + 1)
        arrive(2 * p + 2)

    wait_pair(jnp.int32(0))
    fill(1, odd)

    def box_pair(p, carry):
        k = 2 * p + 1
        fill(k + 1, even)
        geometry(k, odd, False)

        @pl.when(p < 12)
        def _():
            wait_pair(p + 1)

        fill(jnp.minimum(k + 2, 26), odd)
        geometry(k + 1, even, False)
        return carry

    lax.fori_loop(0, 13, box_pair, 0)

    permanent = [jnp.sum(totals[d], axis=0, keepdims=True) for d in range(3)]
    to_shift = jnp.where(live, DRUDE_GAIN * drude, 0.0)
    to_moment = to_shift * drude * (1.0 / CUTOFF**3)

    def induced(turn, boxes, first):
        part_a = part_b = None
        for k in boxes:
            mu = [moments[turn, k, d : d + 1] for d in range(3)]
            at = [places[k, d : d + 1] for d in range(3)]
            along = at[0] * mu[0] + at[1] * mu[1] + at[2] * mu[2]
            rows = mu + [along]
            rows += [mu[d] * at[e] for e in range(3) for d in range(3)]
            rows += [along * at[e] for e in range(3)]
            high, rest = split(jnp.concatenate(rows, axis=0))
            middle, rest = split(rest)
            left = jnp.concatenate([high, middle, rest.astype(BF16)], axis=0)

            def through(coef, part, k=k, left=left):
                high, low = split(coef[k].reshape(SLOTS, SLOTS))
                for right in (high, low.astype(BF16)):
                    term = jnp.dot(left, right, preferred_element_type=F32)
                    part = term if part is None else part + term
                return part

            part_a = through(coef_a, part_a)
            part_b = through(coef_b, part_b)
        if first:
            sums_a[...] = part_a
            sums_b[...] = part_b
        else:
            sums_a[...] += part_a
            sums_b[...] += part_b

    near = jnp.where(lax.rem(mine[2], 4) == 3, 2, 1)

    def choose():
        lane1 = lax.broadcasted_iota(jnp.int32, (1, 128), 1)
        lane = lax.broadcasted_iota(jnp.int32, (MOVE, 128), 1)
        pick = lax.rem(lane, MOVE) == lax.broadcasted_iota(jnp.int32, (MOVE, 128), 0)
        pick = jnp.where(pick, 1.0, 0.0)
        flat = jnp.full((1, 128), -1.0, F32)
        for at in range(6):
            tiled = jnp.dot(
                jnp.broadcast_to(leaving_ref[at].astype(F32), (8, MOVE)),
                pick,
                precision=HIGHEST,
                preferred_element_type=F32,
            )[0:1]
            flat = jnp.where(lane1 // MOVE == at, tiled, flat)
        slot_rows = lax.broadcasted_iota(jnp.int32, (SLOTS, 128), 0).astype(F32)
        chosen[0:SLOTS] = jnp.where(slot_rows == flat, 1.0, 0.0)
        chosen[SLOTS : SLOTS + 8] = jnp.broadcast_to(flat, (8, 128))

    for d in range(3):
        latest[3 + d : 4 + d] = permanent[d]
        latest[6 + d : 7 + d] = permanent[d]

    def turn_body(turn, carry):
        for d in range(3):
            field = latest[3 + d : 4 + d]
            latest[d : d + 1] = field
            moments[turn, 0, d : d + 1] = to_moment * field
        moments[turn, 0, 3:4] = jnp.zeros((1, SLOTS), F32)
        for k in range(26, 0, -1):
            moment_copy(turn, mirror[k], peers[k]).start()
        induced(turn, [0], True)

        @pl.when(turn == 0)
        def _():
            choose()

        landed(moments.at[turn, pl.ds(1, 4)], moment_recv.at[turn, 0])
        induced(turn, [1, 2, 3, 4], False)
        landed(moments.at[turn, pl.ds(5, 4)], moment_recv.at[turn, 1])
        induced(turn, [5, 6, 7, 8], False)
        for side in (near, 3 - near):
            landed(moments.at[turn, pl.ds(side * 9, 9)], moment_recv.at[turn, side + 1])
            induced(turn, [side * 9 + at for at in range(9)], False)
        landed(moments.at[turn, pl.ds(1, 26)], moment_send.at[turn])
        tall, wide = sums_a[...], sums_b[...]
        tall = tall[0:16] + tall[16:32] + tall[32:48]
        wide = wide[0:16] + wide[16:32] + wide[32:48]
        plain = place[0] * tall[0:1] + place[1] * tall[1:2] + place[2] * tall[2:3] - tall[3:4]
        for e in range(3):
            mixed = [place[d] * tall[4 + 3 * e + d : 5 + 3 * e + d] for d in range(3)]
            dipolar = place[e] * plain - (mixed[0] + mixed[1] + mixed[2]) + tall[13 + e : 14 + e]
            latest[3 + e : 4 + e] = latest[6 + e : 7 + e] + 3.0 * dipolar - wide[e : e + 1]
        return carry

    lax.fori_loop(0, ITERS, turn_body, 0)
    before = [latest[d : d + 1] for d in range(3)]
    fields = [latest[3 + d : 4 + d] for d in range(3)]
    shifts = [to_shift * before[d] for d in range(3)]

    mass = masses_ref[0]
    velocity = [velocity_ref[d] + KICK * charge * fields[d] / mass for d in range(3)]
    moved = [fractions[d] + (TIMESTEP / EDGE) * velocity[d] for d in range(3)]
    rows = moved + velocity + shifts
    rest = [charge, drude, screening, label, mass, jnp.zeros((2, SLOTS), F32)]
    complete = jnp.concatenate(rows + rest, axis=0)
    matches = chosen[0:SLOTS]
    flat = chosen[SLOTS : SLOTS + 1]
    packed = jnp.dot(complete, matches, precision=HIGHEST, preferred_element_type=F32)
    present = jnp.where(flat >= 0.0, 1.0, 0.0)
    face = lax.broadcasted_iota(jnp.int32, (1, 128), 1) // MOVE
    headings = []
    for d in range(3):
        heading = jnp.where(face == 2 * d, -1.0, 0.0) + jnp.where(face == 2 * d + 1, 1.0, 0.0)
        headings.append(heading * present)
    headings.append(jnp.zeros((13, 128), F32))
    outbox[...] = packed + jnp.concatenate(headings, axis=0)

    def out_copy(face, device):
        return pltpu.make_async_remote_copy(
            src_ref=outbox,
            dst_ref=inbox.at[face],
            send_sem=out_send,
            recv_sem=out_recv,
            device_id=device,
            device_id_type=MESH,
        )

    for at in range(5, -1, -1):
        out_copy(at, step_from(mine, sizes, UNITS[at])).start()
    named = lax.dot_general(
        jnp.ones((8, 128), F32), matches, (((1,), (1,)), ((), ())), preferred_element_type=F32
    )[0:1]
    remain = jnp.logical_and(live, named < 0.5)
    for at in range(9):
        staying_ref[at] = jnp.where(remain, rows[at], 0.0)
    landed(statics.at[pl.ds(1, 26)], static_send)
    landed(inbox, out_recv)
    result = jnp.zeros((16, 128), F32)
    lane16 = lax.broadcasted_iota(jnp.int32, (16, 128), 1) // MOVE
    for at in range(6):
        result = jnp.where(lane16 == at, inbox[at], result)
    for at in range(14):
        arrivals_ref[at] = result[at : at + 1, 0 : 6 * MOVE]
    landed(inbox, out_send)


def solution(mesh):
    sizes = tuple(mesh.shape[axis] for axis in AXES)
    vec = P("gx", "gy", "gz", None, None)
    row = P("gx", "gy", "gz", None)
    placed = (vec, vec, row, row, row, row, row, P("gx", "gy", "gz"), vec)
    vmem = pl.BlockSpec(memory_space=pltpu.VMEM)
    hbm = pl.BlockSpec(memory_space=pltpu.HBM)
    call = pl.pallas_call(
        functools.partial(kernel, sizes),
        out_shape=(
            jax.ShapeDtypeStruct((9, 1, SLOTS), F32),
            jax.ShapeDtypeStruct((14, 1, 6 * MOVE), F32),
        ),
        in_specs=[hbm] * 9,
        out_specs=(vmem, vmem),
        scratch_shapes=[
            pltpu.VMEM((3, 1, SLOTS), F32),
            pltpu.VMEM((3, 1, SLOTS), F32),
            pltpu.VMEM((1, 1, SLOTS), F32),
            pltpu.VMEM((1, 1, SLOTS), F32),
            pltpu.VMEM((1, 1, SLOTS), F32),
            pltpu.VMEM((1, 1, SLOTS), jnp.int32),
            pltpu.VMEM((1, 1, SLOTS), F32),
            pltpu.VMEM((1, 1, 1), jnp.int32),
            pltpu.VMEM((6, 1, MOVE), jnp.int32),
            pltpu.VMEM((27, 8, SLOTS), F32),
            pltpu.VMEM((27, 4, SLOTS), F32),
            pltpu.VMEM((ITERS, 27, 4, SLOTS), F32),
            pltpu.VMEM((7, GROUPS, 8, 128), F32),
            pltpu.VMEM((7, GROUPS, 8, 128), F32),
            pltpu.VMEM((27, GROUPS, 8, SLOTS), F32),
            pltpu.VMEM((27, GROUPS, 8, SLOTS), F32),
            pltpu.VMEM((3, 8, SLOTS), F32),
            pltpu.VMEM((48, SLOTS), F32),
            pltpu.VMEM((48, SLOTS), F32),
            pltpu.VMEM((SLOTS + 8, 128), F32),
            pltpu.VMEM((16, SLOTS), F32),
            pltpu.VMEM((16, 128), F32),
            pltpu.VMEM((6, 16, 128), F32),
            pltpu.SemaphoreType.DMA((9,)),
            pltpu.SemaphoreType.DMA,
            pltpu.SemaphoreType.DMA((13,)),
            pltpu.SemaphoreType.DMA((ITERS,)),
            pltpu.SemaphoreType.DMA((ITERS, 4)),
            pltpu.SemaphoreType.DMA,
            pltpu.SemaphoreType.DMA,
        ],
        compiler_params=pltpu.CompilerParams(
            collective_id=0, has_side_effects=True, vmem_limit_bytes=67043328
        ),
    )

    def local(fractions, velocity, charge, drude_charge, screening, labels, masses, counts, leaving):
        flat = [value.reshape(1, 1, SLOTS) for value in (charge, drude_charge, screening, labels, masses)]
        staying, arrivals = call(
            fractions.reshape(3, 1, SLOTS),
            velocity.reshape(3, 1, SLOTS),
            *flat,
            counts,
            leaving.reshape(6, 1, MOVE),
        )
        return staying.reshape(1, 1, 1, 9, SLOTS), arrivals.reshape(1, 1, 1, 14, 6 * MOVE)

    return jax.shard_map(local, mesh=mesh, in_specs=placed, out_specs=(vec, vec), check_vma=False)
```

```python
import functools
import math

import jax
import jax.numpy as jnp
from jax import lax
from jax.experimental import pallas as pl
from jax.experimental.pallas import tpu as pltpu
from jax.sharding import PartitionSpec as P

SLOTS = 256
MOVE = 16
ITERS = 3
CUTOFF = 12.0
DRUDE_GAIN = 0.3320636
KICK = 0.002 * 418.4 * 332.0636
TIMESTEP = 0.002
UNITS = ((1, 0, 0), (-1, 0, 0), (0, 1, 0), (0, -1, 0), (0, 0, 1), (0, 0, -1))
EDGE = max(12.0, (10.0 * SLOTS) ** (1.0 / 3.0))
SCALE = EDGE / CUTOFF
LN2 = math.log(2.0)
GROUPS = SLOTS // 8
LAYER = ((0, 0), (1, 0), (-1, 0), (0, 1), (0, -1), (1, 1), (-1, -1), (1, -1), (-1, 1))
CHUNK = 4
AXES = ("gx", "gy", "gz")
MESH = pl.DeviceIdType.MESH
HIGHEST = lax.Precision.HIGHEST
F32 = jnp.float32
BF16 = jnp.bfloat16


def code_offset(code):
    return (code + 1) % 3 - 1 if isinstance(code, int) else lax.rem(code + 1, 3) - 1


def step_from(mine, sizes, step):
    return tuple(lax.rem(mine[a] + (step[a] + sizes[a]), sizes[a]) for a in range(3))


def columns(row):
    return jnp.transpose(jnp.broadcast_to(row, (128, SLOTS))).reshape(GROUPS, 8, 128)


def split(value):
    high = value.astype(BF16)
    return high, value - high.astype(F32)


def kernel(
    sizes,
    fractions_hbm,
    velocity_hbm,
    charge_hbm,
    drude_hbm,
    screening_hbm,
    labels_hbm,
    masses_hbm,
    counts_hbm,
    leaving_hbm,
    staying_ref,
    arrivals_ref,
    fractions_ref,
    velocity_ref,
    charge_ref,
    drude_ref,
    screening_ref,
    labels_ref,
    masses_ref,
    counts_ref,
    leaving_ref,
    statics,
    places,
    moments,
    even,
    odd,
    even_damping,
    odd_damping,
    even_weights,
    odd_weights,
    coef_a,
    coef_b,
    sums_a,
    sums_b,
    chosen,
    latest,
    outbox,
    inbox,
    load_sem,
    static_send,
    static_recv,
    moment_send,
    moment_recv,
    out_send,
    out_recv,
):
    mine = tuple(lax.axis_index(axis) for axis in AXES)
    steps = [(x, y, code_offset(k // 9)) for k, (x, y) in enumerate(LAYER * 3)]
    peers = [step_from(mine, sizes, step) for step in steps]
    mirror = [steps.index((-x, -y, -z)) for x, y, z in steps]

    barrier = pltpu.get_barrier_semaphore()
    for k in range(26, 0, -1):
        pl.semaphore_signal(barrier, inc=1, device_id=peers[k], device_id_type=MESH)

    pairs = (
        (fractions_hbm, fractions_ref),
        (charge_hbm, charge_ref),
        (drude_hbm, drude_ref),
        (screening_hbm, screening_ref),
        (labels_hbm, labels_ref),
        (counts_hbm, counts_ref),
        (velocity_hbm, velocity_ref),
        (masses_hbm, masses_ref),
        (leaving_hbm, leaving_ref),
    )
    loads = [pltpu.make_async_copy(src, dst, load_sem.at[at]) for at, (src, dst) in enumerate(pairs)]
    for load in loads:
        load.start()
    for load in loads:
        load.wait()

    slots = lax.broadcasted_iota(jnp.int32, (1, SLOTS), 1)
    live = slots < jnp.broadcast_to(counts_ref[0], (1, SLOTS))
    fractions = [fractions_ref[d] for d in range(3)]
    charge = jnp.where(live, charge_ref[0], 0.0)
    drude = jnp.where(live, drude_ref[0], -1.0)
    screening = screening_ref[0]
    label = labels_ref[0].astype(F32)
    place = [(fractions[d] - 0.5) * SCALE for d in range(3)]
    root = math.sqrt(0.5 * CUTOFF**3 / LN2) * lax.rsqrt(DRUDE_GAIN * drude * drude)
    own_rows = place + [label, root, screening * root, charge * (1.0 / CUTOFF**2)]
    for at, row in enumerate(own_rows):
        statics[0, at : at + 1] = row
    statics[0, 7:8] = jnp.zeros((1, SLOTS), F32)
    for d in range(3):
        places[0, d : d + 1] = place[d]

    pl.semaphore_wait(barrier, 26)

    def static_copy(slot, device):
        return pltpu.make_async_remote_copy(
            src_ref=statics.at[0],
            dst_ref=statics.at[slot],
            send_sem=static_send,
            recv_sem=static_recv.at[(slot + 1) // 4],
            device_id=device,
            device_id_type=MESH,
        )

    def stage(slot):
        if slot < 9:
            return 0 if slot < 3 else (1 if slot < 5 else 2)
        return 2 * (slot // 9) + (1 if slot % 9 < 5 else 2)

    def moment_copy(turn, slot, device):
        return pltpu.make_async_remote_copy(
            src_ref=moments.at[turn, 0],
            dst_ref=moments.at[turn, slot],
            send_sem=moment_send.at[turn],
            recv_sem=moment_recv.at[turn, stage(slot)],
            device_id=device,
            device_id_type=MESH,
        )

    def landed(ref, sem):
        pltpu.make_async_copy(ref, ref, sem).wait()

    for k in range(26, 0, -1):
        static_copy(mirror[k], peers[k]).start()

    high, rest = split(jnp.concatenate([-screening * root, -root], axis=0))
    low = rest.astype(BF16)
    goal_pairs = jnp.concatenate([high, low, high, low, jnp.zeros((8, SLOTS), BF16)], axis=0)

    def fill(k, buffer, damping):
        def pairs_of():
            high, rest = split(statics[k, 4:6])
            low = rest.astype(BF16)
            pairs = jnp.concatenate([high, high, low, low, jnp.zeros((8, SLOTS), BF16)], axis=0)
            damping[...] = lax.dot_general(
                pairs, goal_pairs, (((0,), (0,)), ((), ())), preferred_element_type=F32
            ).reshape(GROUPS, 8, SLOTS)

        def column_of(at):
            buffer[at] = columns(places[k, at : at + 1] if at < 3 else statics[k, at : at + 1])

        return [pairs_of] + [functools.partial(column_of, at) for at in range(4)]

    def spread(row, half):
        return jnp.broadcast_to(row[:, half * 128 : half * 128 + 128], (8, 128))

    def geometry(k, buffer, damping, weights, own, between=()):
        between = list(between)
        for half in range(2):
            lanes = pl.ds(half * 128, 128)
            goal = [spread(row, half) for row in place + [label]]
            for c in range(GROUPS // CHUNK):
                at = pl.ds(c * CHUNK, CHUNK)
                deltas = [goal[d] - buffer[d, at] for d in range(3)]
                dist_sq = deltas[0] * deltas[0] + deltas[1] * deltas[1] + deltas[2] * deltas[2]
                if own:
                    rows = c * (CHUNK * 8) + lax.broadcasted_iota(jnp.int32, (CHUNK, 8, 128), 0) * 8
                    rows = rows + lax.broadcasted_iota(jnp.int32, (CHUNK, 8, 128), 1)
                    cols = lax.broadcasted_iota(jnp.int32, (CHUNK, 8, 128), 2) + half * 128
                    dist_sq = jnp.where(rows == cols, 1.0, dist_sq)
                inverse = lax.rsqrt(dist_sq)
                inside = jnp.maximum(1.0 - dist_sq, 0.0)
                inverse_sq = inverse * inverse
                radial = (inside * inside) * inverse * inverse_sq
                power = damping[at, :, lanes] * (dist_sq * dist_sq * inverse)
                decay = jnp.exp2(power)
                three = 1.0 - decay
                five = three + (power * LN2) * decay
                direct = radial * three
                coef_b[k, at, :, lanes] = direct
                coef_a[k, at, :, lanes] = radial * inverse_sq * five
                weight = jnp.where(goal[3] != buffer[3, at], direct, 0.0)
                high, rest = split(weight.reshape(CHUNK * 8, 128))
                weights[0, pl.ds(c * CHUNK * 8, CHUNK * 8), lanes] = high
                weights[1, pl.ds(c * CHUNK * 8, CHUNK * 8), lanes] = rest.astype(BF16)
                if between:
                    between.pop(0)()

    def charges(k, weights):
        charge_row = statics[k, 6:7]
        rows = [charge_row] + [charge_row * places[k, d : d + 1] for d in range(3)]
        high, rest = split(jnp.concatenate(rows + [jnp.zeros((12, SLOTS), F32)], axis=0))
        middle, rest = split(rest)
        left = jnp.concatenate([high, middle, rest.astype(BF16)], axis=0)
        part = jnp.dot(left, weights[0], preferred_element_type=F32)
        part += jnp.dot(left, weights[1], preferred_element_type=F32)
        sums_a[...] += part

    def arrive(k):
        at = lax.rem(k, 9)
        sign = jnp.where(lax.rem(at, 2) == 1, SCALE, -SCALE)
        middle = jnp.logical_and(at > 2, at < 5)
        x = jnp.where(jnp.logical_or(at == 0, middle), 0.0, sign)
        y = jnp.where(at < 3, 0.0, jnp.where(at < 7, sign, -sign))
        z = code_offset(k // 9).astype(F32) * SCALE
        for d, moved in enumerate((x, y, z)):
            places[k, d : d + 1] = statics[k, d : d + 1] + moved

    for piece in fill(0, even, even_damping):
        piece()
    geometry(0, even, even_damping, even_weights, True)
    sums_a[...] = jnp.zeros_like(sums_a)

    def run_block(boxes):
        pending = functools.partial(charges, boxes[0] - 1, even_weights)
        held = ((odd, odd_damping, odd_weights), (even, even_damping, even_weights))
        for piece in fill(boxes[0], odd, odd_damping):
            piece()
        for at, k in enumerate(boxes):
            buffer, damping, weights = held[at % 2]
            between = []
            if at + 1 < len(boxes):
                between = fill(boxes[at + 1], *held[(at + 1) % 2][:2])
            geometry(k, buffer, damping, weights, False, between + [pending])
            pending = functools.partial(charges, k, weights)

    landed(statics.at[pl.ds(1, 2)], static_recv.at[0])
    for k in (1, 2):
        arrive(jnp.int32(k))
    run_block([1, 2])

    def box_quad(q, carry):
        base = 4 * q + 3
        landed(statics.at[pl.ds(base, 4)], static_recv.at[q + 1])
        for at in range(4):
            arrive(base + at)
        run_block([base + at for at in range(4)])
        return carry

    lax.fori_loop(0, 6, box_quad, 0)
    charges(26, even_weights)
    tall = sums_a[...]
    tall = tall[0:16] + tall[16:32] + tall[32:48]
    permanent = [place[d] * tall[0:1] - tall[1 + d : 2 + d] for d in range(3)]
    to_shift = jnp.where(live, DRUDE_GAIN * drude, 0.0)
    to_moment = to_shift * drude * (1.0 / CUTOFF**3)

    def induced(turn, boxes, first):
        part_a = part_b = None
        for k in boxes:
            mu = [moments[turn, k, d : d + 1] for d in range(3)]
            at = [places[k, d : d + 1] for d in range(3)]
            along = at[0] * mu[0] + at[1] * mu[1] + at[2] * mu[2]
            rows = mu + [along]
            rows += [mu[d] * at[e] for e in range(3) for d in range(3)]
            rows += [along * at[e] for e in range(3)]
            high, rest = split(jnp.concatenate(rows, axis=0))
            middle, rest = split(rest)
            left = jnp.concatenate([high, middle, rest.astype(BF16)], axis=0)

            def through(coef, part, k=k, left=left):
                high, low = split(coef[k].reshape(SLOTS, SLOTS))
                for right in (high, low.astype(BF16)):
                    term = jnp.dot(left, right, preferred_element_type=F32)
                    part = term if part is None else part + term
                return part

            part_a = through(coef_a, part_a)
            part_b = through(coef_b, part_b)
        if first:
            sums_a[...] = part_a
            sums_b[...] = part_b
        else:
            sums_a[...] += part_a
            sums_b[...] += part_b

    near = jnp.where(lax.rem(mine[2], 4) == 3, 2, 1)

    def choose():
        lane1 = lax.broadcasted_iota(jnp.int32, (1, 128), 1)
        lane = lax.broadcasted_iota(jnp.int32, (MOVE, 128), 1)
        pick = lax.rem(lane, MOVE) == lax.broadcasted_iota(jnp.int32, (MOVE, 128), 0)
        pick = jnp.where(pick, 1.0, 0.0)
        flat = jnp.full((1, 128), -1.0, F32)
        for at in range(6):
            tiled = jnp.dot(
                jnp.broadcast_to(leaving_ref[at].astype(F32), (8, MOVE)),
                pick,
                precision=HIGHEST,
                preferred_element_type=F32,
            )[0:1]
            flat = jnp.where(lane1 // MOVE == at, tiled, flat)
        slot_rows = lax.broadcasted_iota(jnp.int32, (SLOTS, 128), 0).astype(F32)
        chosen[0:SLOTS] = jnp.where(slot_rows == flat, 1.0, 0.0)
        chosen[SLOTS : SLOTS + 8] = jnp.broadcast_to(flat, (8, 128))

    for d in range(3):
        latest[3 + d : 4 + d] = permanent[d]
        latest[6 + d : 7 + d] = permanent[d]

    def turn_body(turn, carry):
        for d in range(3):
            field = latest[3 + d : 4 + d]
            latest[d : d + 1] = field
            moments[turn, 0, d : d + 1] = to_moment * field
        moments[turn, 0, 3:4] = jnp.zeros((1, SLOTS), F32)
        for k in range(26, 0, -1):
            moment_copy(turn, mirror[k], peers[k]).start()
        induced(turn, [0], True)

        @pl.when(turn == 0)
        def _():
            choose()

        landed(moments.at[turn, pl.ds(1, 2)], moment_recv.at[turn, 0])
        induced(turn, [1, 2], False)
        landed(moments.at[turn, pl.ds(3, 2)], moment_recv.at[turn, 1])
        induced(turn, [3, 4], False)
        landed(moments.at[turn, pl.ds(5, 4)], moment_recv.at[turn, 2])
        induced(turn, [5, 6, 7, 8], False)
        for side in (near, 3 - near):
            landed(moments.at[turn, pl.ds(side * 9, 5)], moment_recv.at[turn, 2 * side + 1])
            induced(turn, [side * 9 + at for at in range(5)], False)
            landed(moments.at[turn, pl.ds(side * 9 + 5, 4)], moment_recv.at[turn, 2 * side + 2])
            induced(turn, [side * 9 + at for at in range(5, 9)], False)
        landed(moments.at[turn, pl.ds(1, 26)], moment_send.at[turn])
        tall, wide = sums_a[...], sums_b[...]
        tall = tall[0:16] + tall[16:32] + tall[32:48]
        wide = wide[0:16] + wide[16:32] + wide[32:48]
        plain = place[0] * tall[0:1] + place[1] * tall[1:2] + place[2] * tall[2:3] - tall[3:4]
        for e in range(3):
            mixed = [place[d] * tall[4 + 3 * e + d : 5 + 3 * e + d] for d in range(3)]
            dipolar = place[e] * plain - (mixed[0] + mixed[1] + mixed[2]) + tall[13 + e : 14 + e]
            latest[3 + e : 4 + e] = latest[6 + e : 7 + e] + 3.0 * dipolar - wide[e : e + 1]
        return carry

    lax.fori_loop(0, ITERS, turn_body, 0)
    before = [latest[d : d + 1] for d in range(3)]
    fields = [latest[3 + d : 4 + d] for d in range(3)]
    shifts = [to_shift * before[d] for d in range(3)]

    mass = masses_ref[0]
    velocity = [velocity_ref[d] + KICK * charge * fields[d] / mass for d in range(3)]
    moved = [fractions[d] + (TIMESTEP / EDGE) * velocity[d] for d in range(3)]
    rows = moved + velocity + shifts
    rest = [charge, drude, screening, label, mass, jnp.zeros((2, SLOTS), F32)]
    complete = jnp.concatenate(rows + rest, axis=0)
    matches = chosen[0:SLOTS]
    flat = chosen[SLOTS : SLOTS + 1]
    packed = jnp.dot(complete, matches, precision=HIGHEST, preferred_element_type=F32)
    present = jnp.where(flat >= 0.0, 1.0, 0.0)
    face = lax.broadcasted_iota(jnp.int32, (1, 128), 1) // MOVE
    headings = []
    for d in range(3):
        heading = jnp.where(face == 2 * d, -1.0, 0.0) + jnp.where(face == 2 * d + 1, 1.0, 0.0)
        headings.append(heading * present)
    headings.append(jnp.zeros((13, 128), F32))
    outbox[...] = packed + jnp.concatenate(headings, axis=0)

    def out_copy(face, device):
        return pltpu.make_async_remote_copy(
            src_ref=outbox,
            dst_ref=inbox.at[face],
            send_sem=out_send,
            recv_sem=out_recv,
            device_id=device,
            device_id_type=MESH,
        )

    for at in range(5, -1, -1):
        out_copy(at, step_from(mine, sizes, UNITS[at])).start()
    named = lax.dot_general(
        jnp.ones((8, 128), F32), matches, (((1,), (1,)), ((), ())), preferred_element_type=F32
    )[0:1]
    remain = jnp.logical_and(live, named < 0.5)
    for at in range(9):
        staying_ref[at] = jnp.where(remain, rows[at], 0.0)
    landed(statics.at[pl.ds(1, 26)], static_send)
    landed(inbox, out_recv)
    result = jnp.zeros((16, 128), F32)
    lane16 = lax.broadcasted_iota(jnp.int32, (16, 128), 1) // MOVE
    for at in range(6):
        result = jnp.where(lane16 == at, inbox[at], result)
    for at in range(14):
        arrivals_ref[at] = result[at : at + 1, 0 : 6 * MOVE]
    landed(inbox, out_send)


def solution(mesh):
    sizes = tuple(mesh.shape[axis] for axis in AXES)
    vec = P("gx", "gy", "gz", None, None)
    row = P("gx", "gy", "gz", None)
    placed = (vec, vec, row, row, row, row, row, P("gx", "gy", "gz"), vec)
    vmem = pl.BlockSpec(memory_space=pltpu.VMEM)
    hbm = pl.BlockSpec(memory_space=pltpu.HBM)
    call = pl.pallas_call(
        functools.partial(kernel, sizes),
        out_shape=(
            jax.ShapeDtypeStruct((9, 1, SLOTS), F32),
            jax.ShapeDtypeStruct((14, 1, 6 * MOVE), F32),
        ),
        in_specs=[hbm] * 9,
        out_specs=(vmem, vmem),
        scratch_shapes=[
            pltpu.VMEM((3, 1, SLOTS), F32),
            pltpu.VMEM((3, 1, SLOTS), F32),
            pltpu.VMEM((1, 1, SLOTS), F32),
            pltpu.VMEM((1, 1, SLOTS), F32),
            pltpu.VMEM((1, 1, SLOTS), F32),
            pltpu.VMEM((1, 1, SLOTS), jnp.int32),
            pltpu.VMEM((1, 1, SLOTS), F32),
            pltpu.VMEM((1, 1, 1), jnp.int32),
            pltpu.VMEM((6, 1, MOVE), jnp.int32),
            pltpu.VMEM((27, 8, SLOTS), F32),
            pltpu.VMEM((27, 4, SLOTS), F32),
            pltpu.VMEM((ITERS, 27, 4, SLOTS), F32),
            pltpu.VMEM((4, GROUPS, 8, 128), F32),
            pltpu.VMEM((4, GROUPS, 8, 128), F32),
            pltpu.VMEM((GROUPS, 8, SLOTS), F32),
            pltpu.VMEM((GROUPS, 8, SLOTS), F32),
            pltpu.VMEM((2, SLOTS, SLOTS), BF16),
            pltpu.VMEM((2, SLOTS, SLOTS), BF16),
            pltpu.VMEM((27, GROUPS, 8, SLOTS), F32),
            pltpu.VMEM((27, GROUPS, 8, SLOTS), F32),
            pltpu.VMEM((48, SLOTS), F32),
            pltpu.VMEM((48, SLOTS), F32),
            pltpu.VMEM((SLOTS + 8, 128), F32),
            pltpu.VMEM((16, SLOTS), F32),
            pltpu.VMEM((16, 128), F32),
            pltpu.VMEM((6, 16, 128), F32),
            pltpu.SemaphoreType.DMA((9,)),
            pltpu.SemaphoreType.DMA,
            pltpu.SemaphoreType.DMA((7,)),
            pltpu.SemaphoreType.DMA((ITERS,)),
            pltpu.SemaphoreType.DMA((ITERS, 7)),
            pltpu.SemaphoreType.DMA,
            pltpu.SemaphoreType.DMA,
        ],
        compiler_params=pltpu.CompilerParams(
            collective_id=0, has_side_effects=True, vmem_limit_bytes=67043328
        ),
    )

    def local(fractions, velocity, charge, drude_charge, screening, labels, masses, counts, leaving):
        flat = [value.reshape(1, 1, SLOTS) for value in (charge, drude_charge, screening, labels, masses)]
        staying, arrivals = call(
            fractions.reshape(3, 1, SLOTS),
            velocity.reshape(3, 1, SLOTS),
            *flat,
            counts,
            leaving.reshape(6, 1, MOVE),
        )
        return staying.reshape(1, 1, 1, 9, SLOTS), arrivals.reshape(1, 1, 1, 14, 6 * MOVE)

    return jax.shard_map(local, mesh=mesh, in_specs=placed, out_specs=(vec, vec), check_vma=False)
```

```python
import functools
import math

import jax
import jax.numpy as jnp
from jax import lax
from jax.experimental import pallas as pl
from jax.experimental.pallas import tpu as pltpu
from jax.sharding import PartitionSpec as P

SLOTS = 256
MOVE = 16
ITERS = 3
CUTOFF = 12.0
DRUDE_GAIN = 0.3320636
KICK = 0.002 * 418.4 * 332.0636
TIMESTEP = 0.002
UNITS = ((1, 0, 0), (-1, 0, 0), (0, 1, 0), (0, -1, 0), (0, 0, 1), (0, 0, -1))
EDGE = max(12.0, (10.0 * SLOTS) ** (1.0 / 3.0))
SCALE = EDGE / CUTOFF
LN2 = math.log(2.0)
GROUPS = SLOTS // 8
LAYER = ((0, 0), (1, 0), (-1, 0), (0, 1), (0, -1), (1, 1), (-1, -1), (1, -1), (-1, 1))
CHUNK = 4
AXES = ("gx", "gy", "gz")
MESH = pl.DeviceIdType.MESH
HIGHEST = lax.Precision.HIGHEST
F32 = jnp.float32
BF16 = jnp.bfloat16


def code_offset(code):
    return (code + 1) % 3 - 1 if isinstance(code, int) else lax.rem(code + 1, 3) - 1


def step_from(mine, sizes, step):
    return tuple(lax.rem(mine[a] + (step[a] + sizes[a]), sizes[a]) for a in range(3))


def columns(row):
    return jnp.transpose(jnp.broadcast_to(row, (128, SLOTS))).reshape(GROUPS, 8, 128)


def split(value):
    high = value.astype(BF16)
    return high, value - high.astype(F32)


def kernel(
    sizes,
    fractions_hbm,
    velocity_hbm,
    charge_hbm,
    drude_hbm,
    screening_hbm,
    labels_hbm,
    masses_hbm,
    counts_hbm,
    leaving_hbm,
    staying_ref,
    arrivals_ref,
    fractions_ref,
    velocity_ref,
    charge_ref,
    drude_ref,
    screening_ref,
    labels_ref,
    masses_ref,
    counts_ref,
    leaving_ref,
    statics,
    places,
    moments,
    even,
    odd,
    even_damping,
    odd_damping,
    even_weights,
    odd_weights,
    coef_a,
    coef_b,
    sums_a,
    sums_b,
    chosen,
    listed,
    latest,
    outbox,
    inbox,
    load_sem,
    static_send,
    static_recv,
    moment_send,
    moment_recv,
    out_send,
    out_recv,
):
    mine = tuple(lax.axis_index(axis) for axis in AXES)
    steps = [(x, y, code_offset(k // 9)) for k, (x, y) in enumerate(LAYER * 3)]
    peers = [step_from(mine, sizes, step) for step in steps]
    mirror = [steps.index((-x, -y, -z)) for x, y, z in steps]

    pairs = (
        (fractions_hbm, fractions_ref),
        (charge_hbm, charge_ref),
        (drude_hbm, drude_ref),
        (screening_hbm, screening_ref),
        (labels_hbm, labels_ref),
        (counts_hbm, counts_ref),
        (velocity_hbm, velocity_ref),
        (masses_hbm, masses_ref),
        (leaving_hbm, leaving_ref),
    )
    loads = [pltpu.make_async_copy(src, dst, load_sem.at[at]) for at, (src, dst) in enumerate(pairs)]
    for load in loads:
        load.start()
    barrier = pltpu.get_barrier_semaphore()
    for k in range(1, 27):
        pl.semaphore_signal(barrier, inc=1, device_id=peers[k], device_id_type=MESH)
    for load in loads:
        load.wait()

    slots = lax.broadcasted_iota(jnp.int32, (1, SLOTS), 1)
    live = slots < jnp.broadcast_to(counts_ref[0], (1, SLOTS))
    fractions = [fractions_ref[d] for d in range(3)]
    charge = jnp.where(live, charge_ref[0], 0.0)
    drude = jnp.where(live, drude_ref[0], -1.0)
    screening = screening_ref[0]
    label = labels_ref[0].astype(F32)
    place = [(fractions[d] - 0.5) * SCALE for d in range(3)]
    root = math.sqrt(0.5 * CUTOFF**3 / LN2) * lax.rsqrt(DRUDE_GAIN * drude * drude)
    own_rows = place + [label, root, screening * root, charge * (1.0 / CUTOFF**2)]
    for at, row in enumerate(own_rows):
        statics[0, at : at + 1] = row
    statics[0, 7:8] = jnp.zeros((1, SLOTS), F32)
    for d in range(3):
        places[0, d : d + 1] = place[d]

    pl.semaphore_wait(barrier, 26)

    def stage(slot):
        if slot < 9:
            return 0 if slot < 3 else (1 if slot < 5 else 2)
        return 3 * (slot // 9) + (slot % 9 + 3) // 4

    def static_copy(slot, device):
        return pltpu.make_async_remote_copy(
            src_ref=statics.at[0],
            dst_ref=statics.at[slot],
            send_sem=static_send,
            recv_sem=static_recv.at[stage(slot)],
            device_id=device,
            device_id_type=MESH,
        )

    def moment_copy(turn, slot, device):
        return pltpu.make_async_remote_copy(
            src_ref=moments.at[turn, 0],
            dst_ref=moments.at[turn, slot],
            send_sem=moment_send.at[turn],
            recv_sem=moment_recv.at[turn, stage(slot)],
            device_id=device,
            device_id_type=MESH,
        )

    def landed(ref, sem):
        pltpu.make_async_copy(ref, ref, sem).wait()

    for k in range(1, 27):
        static_copy(mirror[k], peers[k]).start()

    high, rest = split(jnp.concatenate([-screening * root, -root], axis=0))
    low = rest.astype(BF16)
    goal_pairs = jnp.concatenate([high, low, high, low, jnp.zeros((8, SLOTS), BF16)], axis=0)

    def fill(k, buffer, damping):
        def pairs_of():
            high, rest = split(statics[k, 4:6])
            low = rest.astype(BF16)
            pairs = jnp.concatenate([high, high, low, low, jnp.zeros((8, SLOTS), BF16)], axis=0)
            damping[...] = lax.dot_general(
                pairs, goal_pairs, (((0,), (0,)), ((), ())), preferred_element_type=F32
            ).reshape(GROUPS, 8, SLOTS)

        def column_of(at):
            buffer[at] = columns(places[k, at : at + 1] if at < 3 else statics[k, at : at + 1])

        return [pairs_of] + [functools.partial(column_of, at) for at in range(4)]

    def spread(row, half):
        return jnp.broadcast_to(row[:, half * 128 : half * 128 + 128], (8, 128))

    def geometry(k, buffer, damping, weights, own, between=()):
        between = list(between)
        for half in range(2):
            lanes = pl.ds(half * 128, 128)
            goal = [spread(row, half) for row in place + [label]]
            for c in range(GROUPS // CHUNK):
                at = pl.ds(c * CHUNK, CHUNK)
                deltas = [goal[d] - buffer[d, at] for d in range(3)]
                dist_sq = deltas[0] * deltas[0] + deltas[1] * deltas[1] + deltas[2] * deltas[2]
                if own:
                    rows = c * (CHUNK * 8) + lax.broadcasted_iota(jnp.int32, (CHUNK, 8, 128), 0) * 8
                    rows = rows + lax.broadcasted_iota(jnp.int32, (CHUNK, 8, 128), 1)
                    cols = lax.broadcasted_iota(jnp.int32, (CHUNK, 8, 128), 2) + half * 128
                    dist_sq = jnp.where(rows == cols, 1.0, dist_sq)
                inverse = lax.rsqrt(dist_sq)
                inside = jnp.maximum(1.0 - dist_sq, 0.0)
                inverse_sq = inverse * inverse
                radial = (inside * inside) * inverse * inverse_sq
                power = damping[at, :, lanes] * (dist_sq * dist_sq * inverse)
                decay = jnp.exp2(power)
                three = 1.0 - decay
                five = three + (power * LN2) * decay
                direct = radial * three
                coef_b[k, at, :, lanes] = direct
                coef_a[k, at, :, lanes] = radial * inverse_sq * five
                weight = jnp.where(goal[3] != buffer[3, at], direct, 0.0)
                high, rest = split(weight.reshape(CHUNK * 8, 128))
                weights[0, pl.ds(c * CHUNK * 8, CHUNK * 8), lanes] = high
                weights[1, pl.ds(c * CHUNK * 8, CHUNK * 8), lanes] = rest.astype(BF16)
                if between:
                    between.pop(0)()

    def charges(k, weights):
        charge_row = statics[k, 6:7]
        rows = [charge_row] + [charge_row * places[k, d : d + 1] for d in range(3)]
        high, rest = split(jnp.concatenate(rows + [jnp.zeros((12, SLOTS), F32)], axis=0))
        middle, rest = split(rest)
        left = jnp.concatenate([high, middle, rest.astype(BF16)], axis=0)
        part = jnp.dot(left, weights[0], preferred_element_type=F32)
        part += jnp.dot(left, weights[1], preferred_element_type=F32)
        sums_a[...] += part

    def arrive(k):
        at = lax.rem(k, 9)
        sign = jnp.where(lax.rem(at, 2) == 1, SCALE, -SCALE)
        middle = jnp.logical_and(at > 2, at < 5)
        x = jnp.where(jnp.logical_or(at == 0, middle), 0.0, sign)
        y = jnp.where(at < 3, 0.0, jnp.where(at < 7, sign, -sign))
        z = code_offset(k // 9).astype(F32) * SCALE
        for d, moved in enumerate((x, y, z)):
            places[k, d : d + 1] = statics[k, d : d + 1] + moved

    for piece in fill(0, even, even_damping):
        piece()
    geometry(0, even, even_damping, even_weights, True)
    sums_a[...] = jnp.zeros_like(sums_a)

    def run_block(last, boxes):
        pending = functools.partial(charges, last, even_weights)
        held = ((odd, odd_damping, odd_weights), (even, even_damping, even_weights))
        for piece in fill(boxes[0], odd, odd_damping):
            piece()
        for at, k in enumerate(boxes):
            buffer, damping, weights = held[at % 2]
            between = []
            if at + 1 < len(boxes):
                between = fill(boxes[at + 1], *held[(at + 1) % 2][:2])
            geometry(k, buffer, damping, weights, False, between + [pending])
            pending = functools.partial(charges, k, weights)

    near = jnp.where(lax.rem(mine[2], 4) == 3, 2, 1)
    far = 3 - near

    def enter(first, count, where):
        landed(statics.at[pl.ds(first, count)], static_recv.at[where])
        for at in range(count):
            arrive(jnp.int32(first + at))

    enter(1, 2, 0)
    run_block(0, [1, 2])
    enter(3, 2, 1)
    enter(5, 4, 2)
    run_block(2, [3, 4, 5, 6, 7, 8])
    enter(9 * near, 1, 3 * near)
    enter(9 * far, 1, 3 * far)
    run_block(8, [9 * near, 9 * far])

    def side_boxes(turn, last):
        side = jnp.where(turn == 0, near, far)
        enter(9 * side + 1, 4, 3 * side + 1)
        run_block(last, [9 * side + at for at in range(1, 5)])
        enter(9 * side + 5, 4, 3 * side + 2)
        run_block(9 * side + 4, [9 * side + at for at in range(5, 9)])
        return 9 * side + 8

    last = lax.fori_loop(0, 2, side_boxes, 9 * far)
    charges(last, even_weights)
    tall = sums_a[...]
    tall = tall[0:16] + tall[16:32] + tall[32:48]
    permanent = [place[d] * tall[0:1] - tall[1 + d : 2 + d] for d in range(3)]
    to_shift = jnp.where(live, DRUDE_GAIN * drude, 0.0)
    to_moment = to_shift * drude * (1.0 / CUTOFF**3)

    def induced(turn, boxes, first, corners=False):
        part_a = part_b = None
        for k in boxes:
            mu = [moments[turn, k, d : d + 1] for d in range(3)]
            at = [places[k, d : d + 1] for d in range(3)]
            along = at[0] * mu[0] + at[1] * mu[1] + at[2] * mu[2]
            rows = mu + [along]
            rows += [mu[d] * at[e] for e in range(3) for d in range(3)]
            rows += [along * at[e] for e in range(3)]
            high, rest = split(jnp.concatenate(rows, axis=0))
            middle, rest = split(rest)
            left = jnp.concatenate([high, middle, rest.astype(BF16)], axis=0)

            def through(coef, part, k=k, left=left):
                high, low = split(coef[k].reshape(SLOTS, SLOTS))
                for right in (high,) if corners else (high, low.astype(BF16)):
                    term = jnp.dot(left, right, preferred_element_type=F32)
                    part = term if part is None else part + term
                return part

            part_a = through(coef_a, part_a)
            part_b = through(coef_b, part_b)
        if first:
            sums_a[...] = part_a
            sums_b[...] = part_b
        else:
            sums_a[...] += part_a
            sums_b[...] += part_b

    def choose():
        lane1 = lax.broadcasted_iota(jnp.int32, (1, 128), 1)
        lane = lax.broadcasted_iota(jnp.int32, (MOVE, 128), 1)
        pick = lax.rem(lane, MOVE) == lax.broadcasted_iota(jnp.int32, (MOVE, 128), 0)
        pick = jnp.where(pick, 1.0, 0.0)
        flat = jnp.full((1, 128), -1.0, F32)
        for at in range(6):
            tiled = jnp.dot(
                jnp.broadcast_to(leaving_ref[at].astype(F32), (8, MOVE)),
                pick,
                precision=HIGHEST,
                preferred_element_type=F32,
            )[0:1]
            flat = jnp.where(lane1 // MOVE == at, tiled, flat)
        slot_rows = lax.broadcasted_iota(jnp.int32, (SLOTS, 128), 0).astype(F32)
        chosen[...] = jnp.where(slot_rows == flat, 1.0, 0.0).astype(BF16)
        listed[...] = jnp.broadcast_to(flat, (8, 128))

    for d in range(3):
        latest[3 + d : 4 + d] = permanent[d]
        latest[6 + d : 7 + d] = permanent[d]

    def turn_body(turn, carry):
        for d in range(3):
            field = latest[3 + d : 4 + d]
            latest[d : d + 1] = field
            moments[turn, 0, d : d + 1] = to_moment * field
        moments[turn, 0, 3:4] = jnp.zeros((1, SLOTS), F32)
        for k in range(26, 0, -1):
            moment_copy(turn, mirror[k], peers[k]).start()
        induced(turn, [0], True)

        @pl.when(turn == 0)
        def _():
            choose()

        landed(moments.at[turn, pl.ds(1, 2)], moment_recv.at[turn, 0])
        induced(turn, [1, 2], False)
        landed(moments.at[turn, pl.ds(3, 2)], moment_recv.at[turn, 1])
        induced(turn, [3, 4], False)
        landed(moments.at[turn, pl.ds(5, 4)], moment_recv.at[turn, 2])
        induced(turn, [5, 6, 7, 8], False)
        for side in (near, far):
            landed(moments.at[turn, pl.ds(side * 9, 1)], moment_recv.at[turn, 3 * side])
            landed(moments.at[turn, pl.ds(side * 9 + 1, 4)], moment_recv.at[turn, 3 * side + 1])
            induced(turn, [side * 9 + at for at in range(5)], False)
            landed(moments.at[turn, pl.ds(side * 9 + 5, 4)], moment_recv.at[turn, 3 * side + 2])
            induced(turn, [side * 9 + at for at in range(5, 9)], False, True)
        landed(moments.at[turn, pl.ds(1, 26)], moment_send.at[turn])
        tall, wide = sums_a[...], sums_b[...]
        tall = tall[0:16] + tall[16:32] + tall[32:48]
        wide = wide[0:16] + wide[16:32] + wide[32:48]
        plain = place[0] * tall[0:1] + place[1] * tall[1:2] + place[2] * tall[2:3] - tall[3:4]
        for e in range(3):
            mixed = [place[d] * tall[4 + 3 * e + d : 5 + 3 * e + d] for d in range(3)]
            dipolar = place[e] * plain - (mixed[0] + mixed[1] + mixed[2]) + tall[13 + e : 14 + e]
            latest[3 + e : 4 + e] = latest[6 + e : 7 + e] + 3.0 * dipolar - wide[e : e + 1]
        return carry

    lax.fori_loop(0, ITERS, turn_body, 0)
    before = [latest[d : d + 1] for d in range(3)]
    fields = [latest[3 + d : 4 + d] for d in range(3)]
    shifts = [to_shift * before[d] for d in range(3)]

    mass = masses_ref[0]
    velocity = [velocity_ref[d] + KICK * charge * fields[d] / mass for d in range(3)]
    moved = [fractions[d] + (TIMESTEP / EDGE) * velocity[d] for d in range(3)]
    rows = moved + velocity + shifts
    rest = [charge, drude, screening, label, mass, jnp.zeros((2, SLOTS), F32)]
    complete = jnp.concatenate(rows + rest, axis=0)
    matches = chosen[...]
    flat = listed[0:1]
    high, rest = split(complete)
    middle, rest = split(rest)
    left = jnp.concatenate([high, middle, rest.astype(BF16)], axis=0)
    packed = jnp.dot(left, matches, preferred_element_type=F32)
    packed = packed[0:16] + packed[16:32] + packed[32:48]
    present = jnp.where(flat >= 0.0, 1.0, 0.0)
    face = lax.broadcasted_iota(jnp.int32, (1, 128), 1) // MOVE
    headings = []
    for d in range(3):
        heading = jnp.where(face == 2 * d, -1.0, 0.0) + jnp.where(face == 2 * d + 1, 1.0, 0.0)
        headings.append(heading * present)
    headings.append(jnp.zeros((13, 128), F32))
    outbox[...] = packed + jnp.concatenate(headings, axis=0)

    def out_copy(face, device):
        return pltpu.make_async_remote_copy(
            src_ref=outbox,
            dst_ref=inbox.at[face],
            send_sem=out_send,
            recv_sem=out_recv,
            device_id=device,
            device_id_type=MESH,
        )

    for at in range(5, -1, -1):
        out_copy(at, step_from(mine, sizes, UNITS[at])).start()
    named = lax.dot_general(
        jnp.ones((16, 128), BF16), matches, (((1,), (1,)), ((), ())), preferred_element_type=F32
    )[0:1]
    remain = jnp.logical_and(live, named < 0.5)
    for at in range(9):
        staying_ref[at] = jnp.where(remain, rows[at], 0.0)
    landed(statics.at[pl.ds(1, 26)], static_send)
    landed(inbox, out_recv)
    result = jnp.zeros((16, 128), F32)
    lane16 = lax.broadcasted_iota(jnp.int32, (16, 128), 1) // MOVE
    for at in range(6):
        result = jnp.where(lane16 == at, inbox[at], result)
    for at in range(14):
        arrivals_ref[at] = result[at : at + 1, 0 : 6 * MOVE]
    landed(inbox, out_send)


def solution(mesh):
    sizes = tuple(mesh.shape[axis] for axis in AXES)
    vec = P("gx", "gy", "gz", None, None)
    row = P("gx", "gy", "gz", None)
    placed = (vec, vec, row, row, row, row, row, P("gx", "gy", "gz"), vec)
    vmem = pl.BlockSpec(memory_space=pltpu.VMEM)
    hbm = pl.BlockSpec(memory_space=pltpu.HBM)
    call = pl.pallas_call(
        functools.partial(kernel, sizes),
        out_shape=(
            jax.ShapeDtypeStruct((9, 1, SLOTS), F32),
            jax.ShapeDtypeStruct((14, 1, 6 * MOVE), F32),
        ),
        in_specs=[hbm] * 9,
        out_specs=(vmem, vmem),
        scratch_shapes=[
            pltpu.VMEM((3, 1, SLOTS), F32),
            pltpu.VMEM((3, 1, SLOTS), F32),
            pltpu.VMEM((1, 1, SLOTS), F32),
            pltpu.VMEM((1, 1, SLOTS), F32),
            pltpu.VMEM((1, 1, SLOTS), F32),
            pltpu.VMEM((1, 1, SLOTS), jnp.int32),
            pltpu.VMEM((1, 1, SLOTS), F32),
            pltpu.VMEM((1, 1, 1), jnp.int32),
            pltpu.VMEM((6, 1, MOVE), jnp.int32),
            pltpu.VMEM((27, 8, SLOTS), F32),
            pltpu.VMEM((27, 4, SLOTS), F32),
            pltpu.VMEM((ITERS, 27, 4, SLOTS), F32),
            pltpu.VMEM((4, GROUPS, 8, 128), F32),
            pltpu.VMEM((4, GROUPS, 8, 128), F32),
            pltpu.VMEM((GROUPS, 8, SLOTS), F32),
            pltpu.VMEM((GROUPS, 8, SLOTS), F32),
            pltpu.VMEM((2, SLOTS, SLOTS), BF16),
            pltpu.VMEM((2, SLOTS, SLOTS), BF16),
            pltpu.VMEM((27, GROUPS, 8, SLOTS), F32),
            pltpu.VMEM((27, GROUPS, 8, SLOTS), F32),
            pltpu.VMEM((48, SLOTS), F32),
            pltpu.VMEM((48, SLOTS), F32),
            pltpu.VMEM((SLOTS, 128), BF16),
            pltpu.VMEM((8, 128), F32),
            pltpu.VMEM((16, SLOTS), F32),
            pltpu.VMEM((16, 128), F32),
            pltpu.VMEM((6, 16, 128), F32),
            pltpu.SemaphoreType.DMA((9,)),
            pltpu.SemaphoreType.DMA,
            pltpu.SemaphoreType.DMA((9,)),
            pltpu.SemaphoreType.DMA((ITERS,)),
            pltpu.SemaphoreType.DMA((ITERS, 9)),
            pltpu.SemaphoreType.DMA,
            pltpu.SemaphoreType.DMA,
        ],
        compiler_params=pltpu.CompilerParams(
            collective_id=0, has_side_effects=True, vmem_limit_bytes=67043328
        ),
    )

    def local(fractions, velocity, charge, drude_charge, screening, labels, masses, counts, leaving):
        flat = [value.reshape(1, 1, SLOTS) for value in (charge, drude_charge, screening, labels, masses)]
        staying, arrivals = call(
            fractions.reshape(3, 1, SLOTS),
            velocity.reshape(3, 1, SLOTS),
            *flat,
            counts,
            leaving.reshape(6, 1, MOVE),
        )
        return staying.reshape(1, 1, 1, 9, SLOTS), arrivals.reshape(1, 1, 1, 14, 6 * MOVE)

    return jax.shard_map(local, mesh=mesh, in_specs=placed, out_specs=(vec, vec), check_vma=False)
```

```python
import functools
import math

import jax
import jax.numpy as jnp
from jax import lax
from jax.experimental import pallas as pl
from jax.experimental.pallas import tpu as pltpu
from jax.sharding import PartitionSpec as P

SLOTS = 256
MOVE = 16
ITERS = 3
CUTOFF = 12.0
DRUDE_GAIN = 0.3320636
KICK = 0.002 * 418.4 * 332.0636
TIMESTEP = 0.002
UNITS = ((1, 0, 0), (-1, 0, 0), (0, 1, 0), (0, -1, 0), (0, 0, 1), (0, 0, -1))
EDGE = max(12.0, (10.0 * SLOTS) ** (1.0 / 3.0))
SCALE = EDGE / CUTOFF
LN2 = math.log(2.0)
FLOOR = 2e-6
GROUPS = SLOTS // 8
LAYER = ((0, 0), (1, 0), (-1, 0), (0, 1), (0, -1), (1, 1), (-1, -1), (1, -1), (-1, 1))
CHUNK = 4
AXES = ("gx", "gy", "gz")
MESH = pl.DeviceIdType.MESH
HIGHEST = lax.Precision.HIGHEST
F32 = jnp.float32
BF16 = jnp.bfloat16


def code_offset(code):
    return (code + 1) % 3 - 1 if isinstance(code, int) else lax.rem(code + 1, 3) - 1


def step_from(mine, sizes, step):
    return tuple(lax.rem(mine[a] + (step[a] + sizes[a]), sizes[a]) for a in range(3))


def columns(row):
    return jnp.transpose(jnp.broadcast_to(row, (128, SLOTS))).reshape(GROUPS, 8, 128)


def split(value):
    high = value.astype(BF16)
    return high, value - high.astype(F32)


def kernel(
    sizes,
    fractions_hbm,
    velocity_hbm,
    charge_hbm,
    drude_hbm,
    screening_hbm,
    labels_hbm,
    masses_hbm,
    counts_hbm,
    leaving_hbm,
    staying_ref,
    arrivals_ref,
    fractions_ref,
    velocity_ref,
    charge_ref,
    drude_ref,
    screening_ref,
    labels_ref,
    masses_ref,
    counts_ref,
    leaving_ref,
    statics,
    places,
    moments,
    even,
    odd,
    even_squares,
    odd_squares,
    even_damping,
    odd_damping,
    even_weights,
    odd_weights,
    coef_a,
    coef_b,
    sums_a,
    sums_b,
    chosen,
    listed,
    latest,
    outbox,
    inbox,
    load_sem,
    static_send,
    static_recv,
    moment_send,
    moment_recv,
    out_send,
    out_recv,
):
    mine = tuple(lax.axis_index(axis) for axis in AXES)
    steps = [(x, y, code_offset(k // 9)) for k, (x, y) in enumerate(LAYER * 3)]
    peers = [step_from(mine, sizes, step) for step in steps]
    mirror = [steps.index((-x, -y, -z)) for x, y, z in steps]

    pairs = (
        (fractions_hbm, fractions_ref),
        (charge_hbm, charge_ref),
        (drude_hbm, drude_ref),
        (screening_hbm, screening_ref),
        (labels_hbm, labels_ref),
        (counts_hbm, counts_ref),
        (velocity_hbm, velocity_ref),
        (masses_hbm, masses_ref),
        (leaving_hbm, leaving_ref),
    )
    loads = [pltpu.make_async_copy(src, dst, load_sem.at[at]) for at, (src, dst) in enumerate(pairs)]
    for load in loads:
        load.start()
    barrier = pltpu.get_barrier_semaphore()
    for k in range(1, 27):
        pl.semaphore_signal(barrier, inc=1, device_id=peers[k], device_id_type=MESH)
    for load in loads:
        load.wait()

    slots = lax.broadcasted_iota(jnp.int32, (1, SLOTS), 1)
    live = slots < jnp.broadcast_to(counts_ref[0], (1, SLOTS))
    fractions = [fractions_ref[d] for d in range(3)]
    charge = jnp.where(live, charge_ref[0], 0.0)
    drude = jnp.where(live, drude_ref[0], -1.0)
    screening = screening_ref[0]
    label = labels_ref[0].astype(F32)
    place = [(fractions[d] - 0.5) * SCALE for d in range(3)]
    root = math.sqrt(0.5 * CUTOFF**3 / LN2) * lax.rsqrt(DRUDE_GAIN * drude * drude)
    own_rows = place + [label, root, screening * root, charge * (1.0 / CUTOFF**2)]
    for at, row in enumerate(own_rows):
        statics[0, at : at + 1] = row
    statics[0, 7:8] = jnp.zeros((1, SLOTS), F32)
    for d in range(3):
        places[0, d : d + 1] = place[d]

    pl.semaphore_wait(barrier, 26)

    def stage(slot):
        if slot < 9:
            return 0 if slot < 3 else (1 if slot < 5 else 2)
        return 3 * (slot // 9) + (slot % 9 + 3) // 4

    def static_copy(slot, device):
        return pltpu.make_async_remote_copy(
            src_ref=statics.at[0],
            dst_ref=statics.at[slot],
            send_sem=static_send,
            recv_sem=static_recv.at[stage(slot)],
            device_id=device,
            device_id_type=MESH,
        )

    def moment_copy(turn, slot, device):
        return pltpu.make_async_remote_copy(
            src_ref=moments.at[turn, 0],
            dst_ref=moments.at[turn, slot],
            send_sem=moment_send.at[turn],
            recv_sem=moment_recv.at[turn, stage(slot)],
            device_id=device,
            device_id_type=MESH,
        )

    def landed(ref, sem):
        pltpu.make_async_copy(ref, ref, sem).wait()

    for k in range(1, 27):
        static_copy(mirror[k], peers[k]).start()

    high, rest = split(jnp.concatenate([-screening * root, -root], axis=0))
    low = rest.astype(BF16)
    goal_pairs = jnp.concatenate([high, low, high, low, jnp.zeros((8, SLOTS), BF16)], axis=0)

    def parts(rows):
        high, rest = split(rows)
        middle, rest = split(rest)
        return high.astype(F32), middle.astype(F32), rest

    def norm(at):
        return at[0] * at[0] + at[1] * at[1] + at[2] * at[2]

    one = jnp.ones((1, SLOTS), F32)
    none = jnp.zeros((1, SLOTS), F32)
    goal_high, goal_middle, goal_low = parts(jnp.concatenate([-2.0 * at for at in place] + [one], axis=0))
    goal_norm = parts(norm(place))
    blocks = [goal_high, goal_middle, goal_high, goal_middle, goal_low, goal_high]
    blocks += list(goal_norm) + [none, none, none, none, none]
    goal_squares = jnp.concatenate(blocks, axis=0).astype(BF16)

    def fill(k, buffer, squares, damping):
        def squares_of():
            at = [places[k, d : d + 1] for d in range(3)]
            high, middle, low = parts(jnp.concatenate(at + [norm(at)], axis=0))
            rows = [high, high, middle, middle, high, low, one, one, one, none, none, none, none, none]
            left = jnp.concatenate(rows, axis=0).astype(BF16)
            squares[...] = lax.dot_general(
                left, goal_squares, (((0,), (0,)), ((), ())), preferred_element_type=F32
            ).reshape(GROUPS, 8, SLOTS)

        def pairs_of():
            high, rest = split(statics[k, 4:6])
            low = rest.astype(BF16)
            pairs = jnp.concatenate([high, high, low, low, jnp.zeros((8, SLOTS), BF16)], axis=0)
            damping[...] = lax.dot_general(
                pairs, goal_pairs, (((0,), (0,)), ((), ())), preferred_element_type=F32
            ).reshape(GROUPS, 8, SLOTS)

        def column_of():
            buffer[...] = columns(statics[k, 3:4])

        return [squares_of, pairs_of, column_of]

    def spread(row, half):
        return jnp.broadcast_to(row[:, half * 128 : half * 128 + 128], (8, 128))

    def geometry(k, buffer, squares, damping, weights, own, between=()):
        between = list(between)
        for half in range(2):
            lanes = pl.ds(half * 128, 128)
            goal = spread(label, half)
            for c in range(GROUPS // CHUNK):
                at = pl.ds(c * CHUNK, CHUNK)
                dist_sq = jnp.maximum(squares[at, :, lanes], FLOOR)
                if own:
                    rows = c * (CHUNK * 8) + lax.broadcasted_iota(jnp.int32, (CHUNK, 8, 128), 0) * 8
                    rows = rows + lax.broadcasted_iota(jnp.int32, (CHUNK, 8, 128), 1)
                    cols = lax.broadcasted_iota(jnp.int32, (CHUNK, 8, 128), 2) + half * 128
                    dist_sq = jnp.where(rows == cols, 1.0, dist_sq)
                inverse = lax.rsqrt(dist_sq)
                inside = jnp.maximum(1.0 - dist_sq, 0.0)
                inverse_sq = inverse * inverse
                radial = (inside * inside) * inverse * inverse_sq
                power = damping[at, :, lanes] * (dist_sq * dist_sq * inverse)
                decay = jnp.exp2(power)
                three = 1.0 - decay
                five = three + (power * LN2) * decay
                direct = radial * three
                coef_b[k, at, :, lanes] = direct
                coef_a[k, at, :, lanes] = radial * inverse_sq * five
                weight = jnp.where(goal != buffer[at], direct, 0.0)
                high, rest = split(weight.reshape(CHUNK * 8, 128))
                weights[0, pl.ds(c * CHUNK * 8, CHUNK * 8), lanes] = high
                weights[1, pl.ds(c * CHUNK * 8, CHUNK * 8), lanes] = rest.astype(BF16)
                if between:
                    between.pop(0)()

    def charges(k, weights):
        charge_row = statics[k, 6:7]
        rows = [charge_row] + [charge_row * places[k, d : d + 1] for d in range(3)]
        high, rest = split(jnp.concatenate(rows + [jnp.zeros((12, SLOTS), F32)], axis=0))
        middle, rest = split(rest)
        left = jnp.concatenate([high, middle, rest.astype(BF16)], axis=0)
        part = jnp.dot(left, weights[0], preferred_element_type=F32)
        part += jnp.dot(left, weights[1], preferred_element_type=F32)
        sums_a[...] += part

    def arrive(k):
        at = lax.rem(k, 9)
        sign = jnp.where(lax.rem(at, 2) == 1, SCALE, -SCALE)
        middle = jnp.logical_and(at > 2, at < 5)
        x = jnp.where(jnp.logical_or(at == 0, middle), 0.0, sign)
        y = jnp.where(at < 3, 0.0, jnp.where(at < 7, sign, -sign))
        z = code_offset(k // 9).astype(F32) * SCALE
        for d, moved in enumerate((x, y, z)):
            places[k, d : d + 1] = statics[k, d : d + 1] + moved

    for piece in fill(0, even, even_squares, even_damping):
        piece()
    geometry(0, even, even_squares, even_damping, even_weights, True)
    sums_a[...] = jnp.zeros_like(sums_a)

    def run_block(last, boxes):
        pending = functools.partial(charges, last, even_weights)
        held = (
            (odd, odd_squares, odd_damping, odd_weights),
            (even, even_squares, even_damping, even_weights),
        )
        for piece in fill(boxes[0], *held[0][:3]):
            piece()
        for at, k in enumerate(boxes):
            between = []
            if at + 1 < len(boxes):
                between = fill(boxes[at + 1], *held[(at + 1) % 2][:3])
            geometry(k, *held[at % 2], False, between + [pending])
            pending = functools.partial(charges, k, held[at % 2][3])

    near = jnp.where(lax.rem(mine[2], 4) == 3, 2, 1)
    far = 3 - near

    def enter(first, count, where):
        landed(statics.at[pl.ds(first, count)], static_recv.at[where])
        for at in range(count):
            arrive(jnp.int32(first + at))

    enter(1, 2, 0)
    run_block(0, [1, 2])
    enter(3, 2, 1)
    enter(5, 4, 2)
    run_block(2, [3, 4, 5, 6, 7, 8])
    enter(9 * near, 1, 3 * near)
    enter(9 * far, 1, 3 * far)
    run_block(8, [9 * near, 9 * far])

    def side_boxes(turn, last):
        side = jnp.where(turn == 0, near, far)
        enter(9 * side + 1, 4, 3 * side + 1)
        run_block(last, [9 * side + at for at in range(1, 5)])
        enter(9 * side + 5, 4, 3 * side + 2)
        run_block(9 * side + 4, [9 * side + at for at in range(5, 9)])
        return 9 * side + 8

    last = lax.fori_loop(0, 2, side_boxes, 9 * far)
    charges(last, even_weights)
    tall = sums_a[...]
    tall = tall[0:16] + tall[16:32] + tall[32:48]
    permanent = [place[d] * tall[0:1] - tall[1 + d : 2 + d] for d in range(3)]
    to_shift = jnp.where(live, DRUDE_GAIN * drude, 0.0)
    to_moment = to_shift * drude * (1.0 / CUTOFF**3)

    def induced(turn, boxes, first, corners=()):
        part_a = part_b = None
        for k in list(boxes) + list(corners):
            fine = k in boxes if isinstance(k, int) else any(k is box for box in boxes)
            mu = [moments[turn, k, d] for d in range(3)]
            at = [places[k, d : d + 1] for d in range(3)]
            along = at[0] * mu[0] + at[1] * mu[1] + at[2] * mu[2]
            rows = mu + [along]
            rows += [mu[d] * at[e] for e in range(3) for d in range(3)]
            rows += [along * at[e] for e in range(3)]
            high, rest = split(jnp.concatenate(rows, axis=0))
            middle, rest = split(rest)
            left = jnp.concatenate([high, middle, rest.astype(BF16)], axis=0)

            def through(coef, part, k=k, left=left, fine=fine):
                high, low = split(coef[k].reshape(SLOTS, SLOTS))
                for right in (high, low.astype(BF16)) if fine else (high,):
                    term = jnp.dot(left, right, preferred_element_type=F32)
                    part = term if part is None else part + term
                return part

            part_a = through(coef_a, part_a)
            part_b = through(coef_b, part_b)
        if first:
            sums_a[...] = part_a
            sums_b[...] = part_b
        else:
            sums_a[...] += part_a
            sums_b[...] += part_b

    def choose():
        lane1 = lax.broadcasted_iota(jnp.int32, (1, 128), 1)
        lane = lax.broadcasted_iota(jnp.int32, (MOVE, 128), 1)
        pick = lax.rem(lane, MOVE) == lax.broadcasted_iota(jnp.int32, (MOVE, 128), 0)
        pick = jnp.where(pick, 1.0, 0.0)
        flat = jnp.full((1, 128), -1.0, F32)
        for at in range(6):
            tiled = jnp.dot(
                jnp.broadcast_to(leaving_ref[at].astype(F32), (8, MOVE)),
                pick,
                precision=HIGHEST,
                preferred_element_type=F32,
            )[0:1]
            flat = jnp.where(lane1 // MOVE == at, tiled, flat)
        slot_rows = lax.broadcasted_iota(jnp.int32, (SLOTS, 128), 0).astype(F32)
        chosen[...] = jnp.where(slot_rows == flat, 1.0, 0.0).astype(BF16)
        listed[...] = jnp.broadcast_to(flat, (8, 128))

    for d in range(3):
        latest[3 + d : 4 + d] = permanent[d]
        latest[6 + d : 7 + d] = permanent[d]

    def turn_body(turn, carry):
        for d in range(3):
            field = latest[3 + d : 4 + d]
            latest[d : d + 1] = field
            moments[turn, 0, d] = to_moment * field
        for k in range(26, 0, -1):
            moment_copy(turn, mirror[k], peers[k]).start()
        induced(turn, [0], True)

        @pl.when(turn == 0)
        def _():
            choose()

        landed(moments.at[turn, pl.ds(1, 2)], moment_recv.at[turn, 0])
        induced(turn, [1, 2], False)
        landed(moments.at[turn, pl.ds(3, 2)], moment_recv.at[turn, 1])
        induced(turn, [3, 4], False)
        landed(moments.at[turn, pl.ds(5, 4)], moment_recv.at[turn, 2])
        landed(moments.at[turn, pl.ds(near * 9, 1)], moment_recv.at[turn, 3 * near])
        landed(moments.at[turn, pl.ds(near * 9 + 1, 4)], moment_recv.at[turn, 3 * near + 1])
        induced(turn, [5, 6, 7, 8] + [near * 9 + at for at in range(5)], False)
        landed(moments.at[turn, pl.ds(near * 9 + 5, 4)], moment_recv.at[turn, 3 * near + 2])
        landed(moments.at[turn, pl.ds(far * 9, 1)], moment_recv.at[turn, 3 * far])
        landed(moments.at[turn, pl.ds(far * 9 + 1, 4)], moment_recv.at[turn, 3 * far + 1])
        near_corners = [near * 9 + at for at in range(5, 9)]
        induced(turn, [far * 9 + at for at in range(5)], False, near_corners)
        landed(moments.at[turn, pl.ds(far * 9 + 5, 4)], moment_recv.at[turn, 3 * far + 2])
        induced(turn, [], False, [far * 9 + at for at in range(5, 9)])
        landed(moments.at[turn, pl.ds(1, 26)], moment_send.at[turn])
        tall, wide = sums_a[...], sums_b[...]
        tall = tall[0:16] + tall[16:32] + tall[32:48]
        wide = wide[0:16] + wide[16:32] + wide[32:48]
        plain = place[0] * tall[0:1] + place[1] * tall[1:2] + place[2] * tall[2:3] - tall[3:4]
        for e in range(3):
            mixed = [place[d] * tall[4 + 3 * e + d : 5 + 3 * e + d] for d in range(3)]
            dipolar = place[e] * plain - (mixed[0] + mixed[1] + mixed[2]) + tall[13 + e : 14 + e]
            latest[3 + e : 4 + e] = latest[6 + e : 7 + e] + 3.0 * dipolar - wide[e : e + 1]
        return carry

    lax.fori_loop(0, ITERS, turn_body, 0)
    before = [latest[d : d + 1] for d in range(3)]
    fields = [latest[3 + d : 4 + d] for d in range(3)]
    shifts = [to_shift * before[d] for d in range(3)]

    mass = masses_ref[0]
    velocity = [velocity_ref[d] + KICK * charge * fields[d] / mass for d in range(3)]
    moved = [fractions[d] + (TIMESTEP / EDGE) * velocity[d] for d in range(3)]
    rows = moved + velocity + shifts
    rest = [charge, drude, screening, label, mass, jnp.zeros((2, SLOTS), F32)]
    complete = jnp.concatenate(rows + rest, axis=0)
    matches = chosen[...]
    flat = listed[0:1]
    high, rest = split(complete)
    middle, rest = split(rest)
    left = jnp.concatenate([high, middle, rest.astype(BF16)], axis=0)
    packed = jnp.dot(left, matches, preferred_element_type=F32)
    packed = packed[0:16] + packed[16:32] + packed[32:48]
    present = jnp.where(flat >= 0.0, 1.0, 0.0)
    face = lax.broadcasted_iota(jnp.int32, (1, 128), 1) // MOVE
    headings = []
    for d in range(3):
        heading = jnp.where(face == 2 * d, -1.0, 0.0) + jnp.where(face == 2 * d + 1, 1.0, 0.0)
        headings.append(heading * present)
    headings.append(jnp.zeros((13, 128), F32))
    outbox[...] = packed + jnp.concatenate(headings, axis=0)

    def out_copy(face, device):
        return pltpu.make_async_remote_copy(
            src_ref=outbox,
            dst_ref=inbox.at[face],
            send_sem=out_send,
            recv_sem=out_recv,
            device_id=device,
            device_id_type=MESH,
        )

    for at in range(5, -1, -1):
        out_copy(at, step_from(mine, sizes, UNITS[at])).start()
    named = lax.dot_general(
        jnp.ones((16, 128), BF16), matches, (((1,), (1,)), ((), ())), preferred_element_type=F32
    )[0:1]
    remain = jnp.logical_and(live, named < 0.5)
    for at in range(9):
        staying_ref[at] = jnp.where(remain, rows[at], 0.0)
    landed(statics.at[pl.ds(1, 26)], static_send)
    landed(inbox, out_recv)
    result = jnp.zeros((16, 128), F32)
    lane16 = lax.broadcasted_iota(jnp.int32, (16, 128), 1) // MOVE
    for at in range(6):
        result = jnp.where(lane16 == at, inbox[at], result)
    for at in range(14):
        arrivals_ref[at] = result[at : at + 1, 0 : 6 * MOVE]
    landed(inbox, out_send)


def solution(mesh):
    sizes = tuple(mesh.shape[axis] for axis in AXES)
    vec = P("gx", "gy", "gz", None, None)
    row = P("gx", "gy", "gz", None)
    placed = (vec, vec, row, row, row, row, row, P("gx", "gy", "gz"), vec)
    vmem = pl.BlockSpec(memory_space=pltpu.VMEM)
    hbm = pl.BlockSpec(memory_space=pltpu.HBM)
    call = pl.pallas_call(
        functools.partial(kernel, sizes),
        out_shape=(
            jax.ShapeDtypeStruct((9, 1, SLOTS), F32),
            jax.ShapeDtypeStruct((14, 1, 6 * MOVE), F32),
        ),
        in_specs=[hbm] * 9,
        out_specs=(vmem, vmem),
        scratch_shapes=[
            pltpu.VMEM((3, 1, SLOTS), F32),
            pltpu.VMEM((3, 1, SLOTS), F32),
            pltpu.VMEM((1, 1, SLOTS), F32),
            pltpu.VMEM((1, 1, SLOTS), F32),
            pltpu.VMEM((1, 1, SLOTS), F32),
            pltpu.VMEM((1, 1, SLOTS), jnp.int32),
            pltpu.VMEM((1, 1, SLOTS), F32),
            pltpu.VMEM((1, 1, 1), jnp.int32),
            pltpu.VMEM((6, 1, MOVE), jnp.int32),
            pltpu.VMEM((27, 8, SLOTS), F32),
            pltpu.VMEM((27, 4, SLOTS), F32),
            pltpu.VMEM((ITERS, 27, 3, 1, SLOTS), F32),
            pltpu.VMEM((GROUPS, 8, 128), F32),
            pltpu.VMEM((GROUPS, 8, 128), F32),
            pltpu.VMEM((GROUPS, 8, SLOTS), F32),
            pltpu.VMEM((GROUPS, 8, SLOTS), F32),
            pltpu.VMEM((GROUPS, 8, SLOTS), F32),
            pltpu.VMEM((GROUPS, 8, SLOTS), F32),
            pltpu.VMEM((2, SLOTS, SLOTS), BF16),
            pltpu.VMEM((2, SLOTS, SLOTS), BF16),
            pltpu.VMEM((27, GROUPS, 8, SLOTS), F32),
            pltpu.VMEM((27, GROUPS, 8, SLOTS), F32),
            pltpu.VMEM((48, SLOTS), F32),
            pltpu.VMEM((48, SLOTS), F32),
            pltpu.VMEM((SLOTS, 128), BF16),
            pltpu.VMEM((8, 128), F32),
            pltpu.VMEM((16, SLOTS), F32),
            pltpu.VMEM((16, 128), F32),
            pltpu.VMEM((6, 16, 128), F32),
            pltpu.SemaphoreType.DMA((9,)),
            pltpu.SemaphoreType.DMA,
            pltpu.SemaphoreType.DMA((9,)),
            pltpu.SemaphoreType.DMA((ITERS,)),
            pltpu.SemaphoreType.DMA((ITERS, 9)),
            pltpu.SemaphoreType.DMA,
            pltpu.SemaphoreType.DMA,
        ],
        compiler_params=pltpu.CompilerParams(
            collective_id=0, has_side_effects=True, vmem_limit_bytes=67043328
        ),
    )

    def local(fractions, velocity, charge, drude_charge, screening, labels, masses, counts, leaving):
        flat = [value.reshape(1, 1, SLOTS) for value in (charge, drude_charge, screening, labels, masses)]
        staying, arrivals = call(
            fractions.reshape(3, 1, SLOTS),
            velocity.reshape(3, 1, SLOTS),
            *flat,
            counts,
            leaving.reshape(6, 1, MOVE),
        )
        return staying.reshape(1, 1, 1, 9, SLOTS), arrivals.reshape(1, 1, 1, 14, 6 * MOVE)

    return jax.shard_map(local, mesh=mesh, in_specs=placed, out_specs=(vec, vec), check_vma=False)
```

```python
import functools
import math

import jax
import jax.numpy as jnp
from jax import lax
from jax.experimental import pallas as pl
from jax.experimental.pallas import tpu as pltpu
from jax.sharding import PartitionSpec as P

SLOTS = 256
MOVE = 16
ITERS = 3
CUTOFF = 12.0
DRUDE_GAIN = 0.3320636
KICK = 0.002 * 418.4 * 332.0636
TIMESTEP = 0.002
UNITS = ((1, 0, 0), (-1, 0, 0), (0, 1, 0), (0, -1, 0), (0, 0, 1), (0, 0, -1))
EDGE = max(12.0, (10.0 * SLOTS) ** (1.0 / 3.0))
SCALE = EDGE / CUTOFF
LN2 = math.log(2.0)
FLOOR = 2e-6
GROUPS = SLOTS // 8
LAYER = ((0, 0), (1, 0), (-1, 0), (0, 1), (0, -1), (1, 1), (-1, -1), (1, -1), (-1, 1))
CHUNK = 4
AXES = ("gx", "gy", "gz")
MESH = pl.DeviceIdType.MESH
HIGHEST = lax.Precision.HIGHEST
F32 = jnp.float32
BF16 = jnp.bfloat16


def code_offset(code):
    return (code + 1) % 3 - 1 if isinstance(code, int) else lax.rem(code + 1, 3) - 1


def step_from(mine, sizes, step):
    return tuple(lax.rem(mine[a] + (step[a] + sizes[a]), sizes[a]) for a in range(3))


def columns(row):
    return jnp.transpose(jnp.broadcast_to(row, (128, SLOTS))).reshape(GROUPS, 8, 128)


def split(value):
    high = value.astype(BF16)
    return high, value - high.astype(F32)


def kernel(
    sizes,
    fractions_hbm,
    velocity_hbm,
    charge_hbm,
    drude_hbm,
    screening_hbm,
    labels_hbm,
    masses_hbm,
    counts_hbm,
    leaving_hbm,
    staying_ref,
    arrivals_ref,
    fractions_ref,
    velocity_ref,
    charge_ref,
    drude_ref,
    screening_ref,
    labels_ref,
    masses_ref,
    counts_ref,
    leaving_ref,
    statics,
    places,
    moments,
    even,
    odd,
    even_squares,
    odd_squares,
    even_damping,
    odd_damping,
    even_weights,
    odd_weights,
    coef_a,
    coef_b,
    sums_a,
    sums_b,
    chosen,
    listed,
    latest,
    outbox,
    inbox,
    load_sem,
    static_send,
    static_recv,
    moment_send,
    moment_recv,
    out_send,
    out_recv,
):
    mine = tuple(lax.axis_index(axis) for axis in AXES)
    steps = [(x, y, code_offset(k // 9)) for k, (x, y) in enumerate(LAYER * 3)]
    peers = [step_from(mine, sizes, step) for step in steps]
    mirror = [steps.index((-x, -y, -z)) for x, y, z in steps]

    pairs = (
        (fractions_hbm, fractions_ref),
        (charge_hbm, charge_ref),
        (drude_hbm, drude_ref),
        (screening_hbm, screening_ref),
        (labels_hbm, labels_ref),
        (counts_hbm, counts_ref),
        (velocity_hbm, velocity_ref),
        (masses_hbm, masses_ref),
        (leaving_hbm, leaving_ref),
    )
    loads = [pltpu.make_async_copy(src, dst, load_sem.at[at]) for at, (src, dst) in enumerate(pairs)]
    for load in loads:
        load.start()
    barrier = pltpu.get_barrier_semaphore()
    for k in range(1, 27):
        pl.semaphore_signal(barrier, inc=1, device_id=peers[k], device_id_type=MESH)
    for load in loads:
        load.wait()

    slots = lax.broadcasted_iota(jnp.int32, (1, SLOTS), 1)
    live = slots < jnp.broadcast_to(counts_ref[0], (1, SLOTS))
    fractions = [fractions_ref[d] for d in range(3)]
    charge = jnp.where(live, charge_ref[0], 0.0)
    drude = jnp.where(live, drude_ref[0], -1.0)
    screening = screening_ref[0]
    label = labels_ref[0].astype(F32)
    place = [(fractions[d] - 0.5) * SCALE for d in range(3)]
    root = math.sqrt(0.5 * CUTOFF**3 / LN2) * lax.rsqrt(DRUDE_GAIN * drude * drude)
    own_rows = place + [label, root, screening * root, charge * (1.0 / CUTOFF**2)]
    for at, row in enumerate(own_rows):
        statics[0, at : at + 1] = row
    statics[0, 7:8] = jnp.zeros((1, SLOTS), F32)
    for d in range(3):
        places[0, d : d + 1] = place[d]

    pl.semaphore_wait(barrier, 26)

    def stage(slot):
        if slot < 9:
            return 0 if slot < 3 else (1 if slot < 5 else 2)
        return 3 * (slot // 9) + (slot % 9 + 3) // 4

    def static_copy(slot, device):
        return pltpu.make_async_remote_copy(
            src_ref=statics.at[0],
            dst_ref=statics.at[slot],
            send_sem=static_send,
            recv_sem=static_recv.at[stage(slot)],
            device_id=device,
            device_id_type=MESH,
        )

    def moment_copy(turn, slot, device):
        return pltpu.make_async_remote_copy(
            src_ref=moments.at[turn, 0],
            dst_ref=moments.at[turn, slot],
            send_sem=moment_send.at[turn],
            recv_sem=moment_recv.at[turn, stage(slot)],
            device_id=device,
            device_id_type=MESH,
        )

    def landed(ref, sem):
        pltpu.make_async_copy(ref, ref, sem).wait()

    for k in range(1, 27):
        static_copy(mirror[k], peers[k]).start()

    high, rest = split(jnp.concatenate([-screening * root, -root], axis=0))
    low = rest.astype(BF16)
    goal_pairs = jnp.concatenate([high, low, high, low, jnp.zeros((8, SLOTS), BF16)], axis=0)

    def parts(rows):
        high, rest = split(rows)
        middle, rest = split(rest)
        return high.astype(F32), middle.astype(F32), rest

    def norm(at):
        return at[0] * at[0] + at[1] * at[1] + at[2] * at[2]

    one = jnp.ones((1, SLOTS), F32)
    none = jnp.zeros((1, SLOTS), F32)
    goal_high, goal_middle, goal_low = parts(jnp.concatenate([-2.0 * at for at in place] + [one], axis=0))
    goal_norm = parts(norm(place))
    blocks = [goal_high, goal_middle, goal_high, goal_middle, goal_low, goal_high]
    blocks += list(goal_norm) + [none, none, none, none, none]
    goal_squares = jnp.concatenate(blocks, axis=0).astype(BF16)

    def fill(k, buffer, squares, damping):
        def squares_of():
            at = [places[k, d : d + 1] for d in range(3)]
            high, middle, low = parts(jnp.concatenate(at + [norm(at)], axis=0))
            rows = [high, high, middle, middle, high, low, one, one, one, none, none, none, none, none]
            left = jnp.concatenate(rows, axis=0).astype(BF16)
            squares[...] = lax.dot_general(
                left, goal_squares, (((0,), (0,)), ((), ())), preferred_element_type=F32
            ).reshape(GROUPS, 8, SLOTS)

        def pairs_of():
            high, rest = split(statics[k, 4:6])
            low = rest.astype(BF16)
            pairs = jnp.concatenate([high, high, low, low, jnp.zeros((8, SLOTS), BF16)], axis=0)
            damping[...] = lax.dot_general(
                pairs, goal_pairs, (((0,), (0,)), ((), ())), preferred_element_type=F32
            ).reshape(GROUPS, 8, SLOTS)

        def column_of():
            buffer[...] = columns(statics[k, 3:4])

        return [squares_of, pairs_of, column_of]

    def spread(row, half):
        return jnp.broadcast_to(row[:, half * 128 : half * 128 + 128], (8, 128))

    def geometry(k, buffer, squares, damping, weights, own, between=()):
        between = list(between)
        for half in range(2):
            lanes = pl.ds(half * 128, 128)
            goal = spread(label, half)
            for c in range(GROUPS // CHUNK):
                at = pl.ds(c * CHUNK, CHUNK)
                dist_sq = jnp.maximum(squares[at, :, lanes], FLOOR)
                if own:
                    rows = c * (CHUNK * 8) + lax.broadcasted_iota(jnp.int32, (CHUNK, 8, 128), 0) * 8
                    rows = rows + lax.broadcasted_iota(jnp.int32, (CHUNK, 8, 128), 1)
                    cols = lax.broadcasted_iota(jnp.int32, (CHUNK, 8, 128), 2) + half * 128
                    dist_sq = jnp.where(rows == cols, 1.0, dist_sq)
                inverse = lax.rsqrt(dist_sq)
                inside = jnp.maximum(1.0 - dist_sq, 0.0)
                inverse_sq = inverse * inverse
                radial = (inside * inside) * inverse * inverse_sq
                power = damping[at, :, lanes] * (dist_sq * dist_sq * inverse)
                decay = jnp.exp2(power)
                three = 1.0 - decay
                five = three + (power * LN2) * decay
                direct = radial * three
                coef_b[k, at, :, lanes] = direct
                coef_a[k, at, :, lanes] = radial * inverse_sq * five
                weight = jnp.where(goal != buffer[at], direct, 0.0)
                high, rest = split(weight.reshape(CHUNK * 8, 128))
                weights[0, pl.ds(c * CHUNK * 8, CHUNK * 8), lanes] = high
                weights[1, pl.ds(c * CHUNK * 8, CHUNK * 8), lanes] = rest.astype(BF16)
                if between:
                    between.pop(0)()

    def charges(k, weights):
        charge_row = statics[k, 6:7]
        rows = [charge_row] + [charge_row * places[k, d : d + 1] for d in range(3)]
        high, rest = split(jnp.concatenate(rows + [jnp.zeros((12, SLOTS), F32)], axis=0))
        middle, rest = split(rest)
        left = jnp.concatenate([high, middle, rest.astype(BF16)], axis=0)
        part = jnp.dot(left, weights[0], preferred_element_type=F32)
        part += jnp.dot(left, weights[1], preferred_element_type=F32)
        sums_a[...] += part

    def arrive(k):
        at = lax.rem(k, 9)
        sign = jnp.where(lax.rem(at, 2) == 1, SCALE, -SCALE)
        middle = jnp.logical_and(at > 2, at < 5)
        x = jnp.where(jnp.logical_or(at == 0, middle), 0.0, sign)
        y = jnp.where(at < 3, 0.0, jnp.where(at < 7, sign, -sign))
        z = code_offset(k // 9).astype(F32) * SCALE
        for d, moved in enumerate((x, y, z)):
            places[k, d : d + 1] = statics[k, d : d + 1] + moved

    for piece in fill(0, even, even_squares, even_damping):
        piece()
    geometry(0, even, even_squares, even_damping, even_weights, True)
    sums_a[...] = jnp.zeros_like(sums_a)

    def run_block(last, boxes):
        pending = functools.partial(charges, last, even_weights)
        held = (
            (odd, odd_squares, odd_damping, odd_weights),
            (even, even_squares, even_damping, even_weights),
        )
        for piece in fill(boxes[0], *held[0][:3]):
            piece()
        for at, k in enumerate(boxes):
            between = []
            if at + 1 < len(boxes):
                between = fill(boxes[at + 1], *held[(at + 1) % 2][:3])
            geometry(k, *held[at % 2], False, between + [pending])
            pending = functools.partial(charges, k, held[at % 2][3])

    near = jnp.where(lax.rem(mine[2], 4) == 3, 2, 1)
    far = 3 - near

    def enter(first, count, where):
        landed(statics.at[pl.ds(first, count)], static_recv.at[where])
        for at in range(count):
            arrive(jnp.int32(first + at))

    enter(1, 2, 0)
    run_block(0, [1, 2])
    enter(3, 2, 1)
    enter(5, 4, 2)
    run_block(2, [3, 4, 5, 6, 7, 8])
    enter(9 * near, 1, 3 * near)
    enter(9 * far, 1, 3 * far)
    run_block(8, [9 * near, 9 * far])

    def side_boxes(turn, last):
        side = jnp.where(turn == 0, near, far)
        enter(9 * side + 1, 4, 3 * side + 1)
        run_block(last, [9 * side + at for at in range(1, 5)])
        enter(9 * side + 5, 4, 3 * side + 2)
        run_block(9 * side + 4, [9 * side + at for at in range(5, 9)])
        return 9 * side + 8

    last = lax.fori_loop(0, 2, side_boxes, 9 * far)
    charges(last, even_weights)
    tall = sums_a[...]
    tall = tall[0:16] + tall[16:32] + tall[32:48]
    permanent = [place[d] * tall[0:1] - tall[1 + d : 2 + d] for d in range(3)]
    to_shift = jnp.where(live, DRUDE_GAIN * drude, 0.0)
    to_moment = to_shift * drude * (1.0 / CUTOFF**3)

    def induced(turn, boxes, first, corners=()):
        part_a = part_b = None
        for k in list(boxes) + list(corners):
            fine = k in boxes if isinstance(k, int) else any(k is box for box in boxes)
            mu = [moments[turn, k, d] for d in range(3)]
            at = [places[k, d : d + 1] for d in range(3)]
            along = at[0] * mu[0] + at[1] * mu[1] + at[2] * mu[2]
            rows = mu + [along]
            rows += [mu[d] * at[e] for e in range(3) for d in range(3)]
            rows += [along * at[e] for e in range(3)]
            high, rest = split(jnp.concatenate(rows, axis=0))
            middle, rest = split(rest)
            left = jnp.concatenate([high, middle, rest.astype(BF16)], axis=0)

            def through(coef, part, k=k, left=left, fine=fine):
                high, low = split(coef[k].reshape(SLOTS, SLOTS))
                for right in (high, low.astype(BF16)) if fine else (high,):
                    term = jnp.dot(left, right, preferred_element_type=F32)
                    part = term if part is None else part + term
                return part

            part_a = through(coef_a, part_a)
            part_b = through(coef_b, part_b)
        if first:
            sums_a[...] = part_a
            sums_b[...] = part_b
        else:
            sums_a[...] += part_a
            sums_b[...] += part_b

    def choose():
        lane1 = lax.broadcasted_iota(jnp.int32, (1, 128), 1)
        lane = lax.broadcasted_iota(jnp.int32, (MOVE, 128), 1)
        pick = lax.rem(lane, MOVE) == lax.broadcasted_iota(jnp.int32, (MOVE, 128), 0)
        pick = jnp.where(pick, 1.0, 0.0)
        flat = jnp.full((1, 128), -1.0, F32)
        for at in range(6):
            tiled = jnp.dot(
                jnp.broadcast_to(leaving_ref[at].astype(F32), (8, MOVE)),
                pick,
                precision=HIGHEST,
                preferred_element_type=F32,
            )[0:1]
            flat = jnp.where(lane1 // MOVE == at, tiled, flat)
        slot_rows = lax.broadcasted_iota(jnp.int32, (SLOTS, 128), 0).astype(F32)
        chosen[...] = jnp.where(slot_rows == flat, 1.0, 0.0).astype(BF16)
        listed[...] = jnp.broadcast_to(flat, (8, 128))

    for d in range(3):
        latest[3 + d : 4 + d] = permanent[d]
        latest[6 + d : 7 + d] = permanent[d]

    def turn_body(turn, carry):
        for d in range(3):
            field = latest[3 + d : 4 + d]
            latest[d : d + 1] = field
            moments[turn, 0, d] = to_moment * field
        for k in [1, 2] + list(range(26, 2, -1)):
            moment_copy(turn, mirror[k], peers[k]).start()
        induced(turn, [0], True)

        @pl.when(turn == 0)
        def _():
            choose()

        landed(moments.at[turn, pl.ds(1, 2)], moment_recv.at[turn, 0])
        induced(turn, [1, 2], False)
        landed(moments.at[turn, pl.ds(3, 2)], moment_recv.at[turn, 1])
        induced(turn, [3, 4], False)
        landed(moments.at[turn, pl.ds(5, 4)], moment_recv.at[turn, 2])
        landed(moments.at[turn, pl.ds(near * 9, 1)], moment_recv.at[turn, 3 * near])
        landed(moments.at[turn, pl.ds(near * 9 + 1, 4)], moment_recv.at[turn, 3 * near + 1])
        induced(turn, [5, 6, 7, 8] + [near * 9 + at for at in range(5)], False)
        landed(moments.at[turn, pl.ds(near * 9 + 5, 4)], moment_recv.at[turn, 3 * near + 2])
        landed(moments.at[turn, pl.ds(far * 9, 1)], moment_recv.at[turn, 3 * far])
        landed(moments.at[turn, pl.ds(far * 9 + 1, 4)], moment_recv.at[turn, 3 * far + 1])
        near_corners = [near * 9 + at for at in range(5, 9)]
        induced(turn, [far * 9 + at for at in range(5)], False, near_corners)
        landed(moments.at[turn, pl.ds(far * 9 + 5, 4)], moment_recv.at[turn, 3 * far + 2])
        induced(turn, [], False, [far * 9 + at for at in range(5, 9)])
        landed(moments.at[turn, pl.ds(1, 26)], moment_send.at[turn])
        tall, wide = sums_a[...], sums_b[...]
        tall = tall[0:16] + tall[16:32] + tall[32:48]
        wide = wide[0:16] + wide[16:32] + wide[32:48]
        plain = place[0] * tall[0:1] + place[1] * tall[1:2] + place[2] * tall[2:3] - tall[3:4]
        for e in range(3):
            mixed = [place[d] * tall[4 + 3 * e + d : 5 + 3 * e + d] for d in range(3)]
            dipolar = place[e] * plain - (mixed[0] + mixed[1] + mixed[2]) + tall[13 + e : 14 + e]
            latest[3 + e : 4 + e] = latest[6 + e : 7 + e] + 3.0 * dipolar - wide[e : e + 1]
        return carry

    lax.fori_loop(0, ITERS, turn_body, 0)
    before = [latest[d : d + 1] for d in range(3)]
    fields = [latest[3 + d : 4 + d] for d in range(3)]
    shifts = [to_shift * before[d] for d in range(3)]

    mass = masses_ref[0]
    velocity = [velocity_ref[d] + KICK * charge * fields[d] / mass for d in range(3)]
    moved = [fractions[d] + (TIMESTEP / EDGE) * velocity[d] for d in range(3)]
    rows = moved + velocity + shifts
    rest = [charge, drude, screening, label, mass, jnp.zeros((2, SLOTS), F32)]
    complete = jnp.concatenate(rows + rest, axis=0)
    matches = chosen[...]
    flat = listed[0:1]
    high, rest = split(complete)
    middle, rest = split(rest)
    left = jnp.concatenate([high, middle, rest.astype(BF16)], axis=0)
    packed = jnp.dot(left, matches, preferred_element_type=F32)
    packed = packed[0:16] + packed[16:32] + packed[32:48]
    present = jnp.where(flat >= 0.0, 1.0, 0.0)
    face = lax.broadcasted_iota(jnp.int32, (1, 128), 1) // MOVE
    headings = []
    for d in range(3):
        heading = jnp.where(face == 2 * d, -1.0, 0.0) + jnp.where(face == 2 * d + 1, 1.0, 0.0)
        headings.append(heading * present)
    headings.append(jnp.zeros((13, 128), F32))
    outbox[...] = packed + jnp.concatenate(headings, axis=0)

    def out_copy(face, device):
        return pltpu.make_async_remote_copy(
            src_ref=outbox,
            dst_ref=inbox.at[face],
            send_sem=out_send,
            recv_sem=out_recv,
            device_id=device,
            device_id_type=MESH,
        )

    for at in range(5, -1, -1):
        out_copy(at, step_from(mine, sizes, UNITS[at])).start()
    named = lax.dot_general(
        jnp.ones((16, 128), BF16), matches, (((1,), (1,)), ((), ())), preferred_element_type=F32
    )[0:1]
    remain = jnp.logical_and(live, named < 0.5)
    for at in range(9):
        staying_ref[at] = jnp.where(remain, rows[at], 0.0)
    landed(statics.at[pl.ds(1, 26)], static_send)
    landed(inbox, out_recv)
    result = jnp.zeros((16, 128), F32)
    lane16 = lax.broadcasted_iota(jnp.int32, (16, 128), 1) // MOVE
    for at in range(6):
        result = jnp.where(lane16 == at, inbox[at], result)
    for at in range(14):
        arrivals_ref[at] = result[at : at + 1, 0 : 6 * MOVE]
    landed(inbox, out_send)


def solution(mesh):
    sizes = tuple(mesh.shape[axis] for axis in AXES)
    vec = P("gx", "gy", "gz", None, None)
    row = P("gx", "gy", "gz", None)
    placed = (vec, vec, row, row, row, row, row, P("gx", "gy", "gz"), vec)
    vmem = pl.BlockSpec(memory_space=pltpu.VMEM)
    hbm = pl.BlockSpec(memory_space=pltpu.HBM)
    call = pl.pallas_call(
        functools.partial(kernel, sizes),
        out_shape=(
            jax.ShapeDtypeStruct((9, 1, SLOTS), F32),
            jax.ShapeDtypeStruct((14, 1, 6 * MOVE), F32),
        ),
        in_specs=[hbm] * 7 + [pl.BlockSpec(memory_space=pl.ANY), hbm],
        out_specs=(vmem, vmem),
        scratch_shapes=[
            pltpu.VMEM((3, 1, SLOTS), F32),
            pltpu.VMEM((3, 1, SLOTS), F32),
            pltpu.VMEM((1, 1, SLOTS), F32),
            pltpu.VMEM((1, 1, SLOTS), F32),
            pltpu.VMEM((1, 1, SLOTS), F32),
            pltpu.VMEM((1, 1, SLOTS), jnp.int32),
            pltpu.VMEM((1, 1, SLOTS), F32),
            pltpu.VMEM((1, 1, 1), jnp.int32),
            pltpu.VMEM((6, 1, MOVE), jnp.int32),
            pltpu.VMEM((27, 8, SLOTS), F32),
            pltpu.VMEM((27, 4, SLOTS), F32),
            pltpu.VMEM((ITERS, 27, 3, 1, SLOTS), F32),
            pltpu.VMEM((GROUPS, 8, 128), F32),
            pltpu.VMEM((GROUPS, 8, 128), F32),
            pltpu.VMEM((GROUPS, 8, SLOTS), F32),
            pltpu.VMEM((GROUPS, 8, SLOTS), F32),
            pltpu.VMEM((GROUPS, 8, SLOTS), F32),
            pltpu.VMEM((GROUPS, 8, SLOTS), F32),
            pltpu.VMEM((2, SLOTS, SLOTS), BF16),
            pltpu.VMEM((2, SLOTS, SLOTS), BF16),
            pltpu.VMEM((27, GROUPS, 8, SLOTS), F32),
            pltpu.VMEM((27, GROUPS, 8, SLOTS), F32),
            pltpu.VMEM((48, SLOTS), F32),
            pltpu.VMEM((48, SLOTS), F32),
            pltpu.VMEM((SLOTS, 128), BF16),
            pltpu.VMEM((8, 128), F32),
            pltpu.VMEM((16, SLOTS), F32),
            pltpu.VMEM((16, 128), F32),
            pltpu.VMEM((6, 16, 128), F32),
            pltpu.SemaphoreType.DMA((9,)),
            pltpu.SemaphoreType.DMA,
            pltpu.SemaphoreType.DMA((9,)),
            pltpu.SemaphoreType.DMA((ITERS,)),
            pltpu.SemaphoreType.DMA((ITERS, 9)),
            pltpu.SemaphoreType.DMA,
            pltpu.SemaphoreType.DMA,
        ],
        compiler_params=pltpu.CompilerParams(
            collective_id=0, has_side_effects=True, vmem_limit_bytes=48 * 1024 * 1024
        ),
    )

    def local(fractions, velocity, charge, drude_charge, screening, labels, masses, counts, leaving):
        flat = [value.reshape(1, 1, SLOTS) for value in (charge, drude_charge, screening, labels, masses)]
        operands = [fractions.reshape(3, 1, SLOTS), velocity.reshape(3, 1, SLOTS), *flat, counts]
        operands.append(leaving.reshape(6, 1, MOVE))
        operands = [value if value.size == 1 else pltpu.with_memory_space_constraint(value, pltpu.HBM) for value in operands]
        staying, arrivals = call(*operands)
        return staying.reshape(1, 1, 1, 9, SLOTS), arrivals.reshape(1, 1, 1, 14, 6 * MOVE)

    return jax.shard_map(local, mesh=mesh, in_specs=placed, out_specs=(vec, vec), check_vma=False)
```

```python
import functools
import math

import jax
import jax.numpy as jnp
from jax import lax
from jax.experimental import pallas as pl
from jax.experimental.pallas import tpu as pltpu
from jax.sharding import PartitionSpec as P

SLOTS = 256
MOVE = 16
ITERS = 3
CUTOFF = 12.0
DRUDE_GAIN = 0.3320636
KICK = 0.002 * 418.4 * 332.0636
TIMESTEP = 0.002
UNITS = ((1, 0, 0), (-1, 0, 0), (0, 1, 0), (0, -1, 0), (0, 0, 1), (0, 0, -1))
EDGE = max(12.0, (10.0 * SLOTS) ** (1.0 / 3.0))
SCALE = EDGE / CUTOFF
LN2 = math.log(2.0)
FLOOR = 2e-6
GROUPS = SLOTS // 8
LAYER = ((0, 0), (1, 0), (-1, 0), (0, 1), (0, -1), (1, 1), (-1, -1), (1, -1), (-1, 1))
CHUNK = 4
AXES = ("gx", "gy", "gz")
MESH = pl.DeviceIdType.MESH
HIGHEST = lax.Precision.HIGHEST
F32 = jnp.float32
BF16 = jnp.bfloat16


def code_offset(code):
    return (code + 1) % 3 - 1 if isinstance(code, int) else lax.rem(code + 1, 3) - 1


def step_from(mine, sizes, step):
    return tuple(lax.rem(mine[a] + (step[a] + sizes[a]), sizes[a]) for a in range(3))


def columns(row):
    return jnp.transpose(jnp.broadcast_to(row, (128, SLOTS))).reshape(GROUPS, 8, 128)


def split(value):
    high = value.astype(BF16)
    return high, value - high.astype(F32)


def kernel(
    sizes,
    fractions_hbm,
    velocity_hbm,
    charge_hbm,
    drude_hbm,
    screening_hbm,
    labels_hbm,
    masses_hbm,
    counts_hbm,
    leaving_hbm,
    staying_ref,
    arrivals_ref,
    fractions_ref,
    velocity_ref,
    charge_ref,
    drude_ref,
    screening_ref,
    labels_ref,
    masses_ref,
    counts_ref,
    leaving_ref,
    statics,
    places,
    moments,
    even,
    odd,
    even_squares,
    odd_squares,
    even_damping,
    odd_damping,
    even_weights,
    odd_weights,
    coef_a,
    coef_b,
    sums_a,
    sums_b,
    chosen,
    listed,
    latest,
    outbox,
    inbox,
    load_sem,
    static_send,
    static_recv,
    moment_send,
    moment_recv,
    out_send,
    out_recv,
):
    mine = tuple(lax.axis_index(axis) for axis in AXES)
    steps = [(x, y, code_offset(k // 9)) for k, (x, y) in enumerate(LAYER * 3)]
    peers = [step_from(mine, sizes, step) for step in steps]
    mirror = [steps.index((-x, -y, -z)) for x, y, z in steps]

    pairs = (
        (fractions_hbm, fractions_ref),
        (charge_hbm, charge_ref),
        (drude_hbm, drude_ref),
        (screening_hbm, screening_ref),
        (labels_hbm, labels_ref),
        (counts_hbm, counts_ref),
        (velocity_hbm, velocity_ref),
        (masses_hbm, masses_ref),
        (leaving_hbm, leaving_ref),
    )
    loads = [pltpu.make_async_copy(src, dst, load_sem.at[at]) for at, (src, dst) in enumerate(pairs)]
    for load in loads:
        load.start()
    barrier = pltpu.get_barrier_semaphore()
    for k in range(1, 27):
        pl.semaphore_signal(barrier, inc=1, device_id=peers[k], device_id_type=MESH)
    for load in loads:
        load.wait()

    slots = lax.broadcasted_iota(jnp.int32, (1, SLOTS), 1)
    live = slots < jnp.broadcast_to(counts_ref[0], (1, SLOTS))
    fractions = [fractions_ref[d] for d in range(3)]
    charge = jnp.where(live, charge_ref[0], 0.0)
    drude = jnp.where(live, drude_ref[0], -1.0)
    screening = screening_ref[0]
    label = labels_ref[0].astype(F32)
    place = [(fractions[d] - 0.5) * SCALE for d in range(3)]
    root = math.sqrt(0.5 * CUTOFF**3 / LN2) * lax.rsqrt(DRUDE_GAIN * drude * drude)
    own_rows = place + [label, root, screening * root, charge * (1.0 / CUTOFF**2)]
    for at, row in enumerate(own_rows):
        statics[0, at : at + 1] = row
    statics[0, 7:8] = jnp.zeros((1, SLOTS), F32)
    for d in range(3):
        places[0, d : d + 1] = place[d]

    pl.semaphore_wait(barrier, 26)

    def stage(slot):
        if slot < 9:
            return 0 if slot < 3 else (1 if slot < 5 else 2)
        return 3 * (slot // 9) + (slot % 9 + 3) // 4

    def static_copy(slot, device):
        return pltpu.make_async_remote_copy(
            src_ref=statics.at[0],
            dst_ref=statics.at[slot],
            send_sem=static_send,
            recv_sem=static_recv.at[stage(slot)],
            device_id=device,
            device_id_type=MESH,
        )

    def moment_copy(turn, slot, device):
        return pltpu.make_async_remote_copy(
            src_ref=moments.at[turn, 0],
            dst_ref=moments.at[turn, slot],
            send_sem=moment_send.at[turn],
            recv_sem=moment_recv.at[turn, stage(slot)],
            device_id=device,
            device_id_type=MESH,
        )

    def landed(ref, sem):
        pltpu.make_async_copy(ref, ref, sem).wait()

    for k in range(1, 27):
        static_copy(mirror[k], peers[k]).start()

    high, rest = split(jnp.concatenate([-screening * root, -root], axis=0))
    low = rest.astype(BF16)
    goal_pairs = jnp.concatenate([high, low, high, low, jnp.zeros((8, SLOTS), BF16)], axis=0)

    def parts(rows):
        high, rest = split(rows)
        middle, rest = split(rest)
        return high.astype(F32), middle.astype(F32), rest

    def norm(at):
        return at[0] * at[0] + at[1] * at[1] + at[2] * at[2]

    one = jnp.ones((1, SLOTS), F32)
    none = jnp.zeros((1, SLOTS), F32)
    goal_high, goal_middle, goal_low = parts(jnp.concatenate([-2.0 * at for at in place] + [one], axis=0))
    goal_norm = parts(norm(place))
    blocks = [goal_high, goal_middle, goal_high, goal_middle, goal_low, goal_high]
    blocks += list(goal_norm) + [none, none, none, none, none]
    goal_squares = jnp.concatenate(blocks, axis=0).astype(BF16)

    def fill(k, buffer, squares, damping):
        def squares_of():
            at = [places[k, d : d + 1] for d in range(3)]
            high, middle, low = parts(jnp.concatenate(at + [norm(at)], axis=0))
            rows = [high, high, middle, middle, high, low, one, one, one, none, none, none, none, none]
            left = jnp.concatenate(rows, axis=0).astype(BF16)
            squares[...] = lax.dot_general(
                left, goal_squares, (((0,), (0,)), ((), ())), preferred_element_type=F32
            ).reshape(GROUPS, 8, SLOTS)

        def pairs_of():
            high, rest = split(statics[k, 4:6])
            low = rest.astype(BF16)
            pairs = jnp.concatenate([high, high, low, low, jnp.zeros((8, SLOTS), BF16)], axis=0)
            damping[...] = lax.dot_general(
                pairs, goal_pairs, (((0,), (0,)), ((), ())), preferred_element_type=F32
            ).reshape(GROUPS, 8, SLOTS)

        def column_of():
            buffer[...] = columns(statics[k, 3:4])

        return [squares_of, pairs_of, column_of]

    def spread(row, half):
        return jnp.broadcast_to(row[:, half * 128 : half * 128 + 128], (8, 128))

    def geometry(k, buffer, squares, damping, weights, own, between=()):
        between = list(between)
        for half in range(2):
            lanes = pl.ds(half * 128, 128)
            goal = spread(label, half)
            for c in range(GROUPS // CHUNK):
                at = pl.ds(c * CHUNK, CHUNK)
                dist_sq = jnp.maximum(squares[at, :, lanes], FLOOR)
                if own:
                    rows = c * (CHUNK * 8) + lax.broadcasted_iota(jnp.int32, (CHUNK, 8, 128), 0) * 8
                    rows = rows + lax.broadcasted_iota(jnp.int32, (CHUNK, 8, 128), 1)
                    cols = lax.broadcasted_iota(jnp.int32, (CHUNK, 8, 128), 2) + half * 128
                    dist_sq = jnp.where(rows == cols, 1.0, dist_sq)
                inverse = lax.rsqrt(dist_sq)
                inside = jnp.maximum(1.0 - dist_sq, 0.0)
                inverse_sq = inverse * inverse
                radial = (inside * inside) * inverse * inverse_sq
                power = damping[at, :, lanes] * (dist_sq * dist_sq * inverse)
                decay = jnp.exp2(power)
                three = 1.0 - decay
                five = three + (power * LN2) * decay
                direct = radial * three
                coef_b[k, at, :, lanes] = direct
                coef_a[k, at, :, lanes] = radial * inverse_sq * five
                weight = jnp.where(goal != buffer[at], direct, 0.0)
                high, rest = split(weight.reshape(CHUNK * 8, 128))
                weights[0, pl.ds(c * CHUNK * 8, CHUNK * 8), lanes] = high
                weights[1, pl.ds(c * CHUNK * 8, CHUNK * 8), lanes] = rest.astype(BF16)
                if between:
                    between.pop(0)()

    def charges(k, weights):
        charge_row = statics[k, 6:7]
        rows = [charge_row] + [charge_row * places[k, d : d + 1] for d in range(3)]
        high, rest = split(jnp.concatenate(rows + [jnp.zeros((12, SLOTS), F32)], axis=0))
        middle, rest = split(rest)
        left = jnp.concatenate([high, middle, rest.astype(BF16)], axis=0)
        part = jnp.dot(left, weights[0], preferred_element_type=F32)
        part += jnp.dot(left, weights[1], preferred_element_type=F32)
        sums_a[...] += part

    def arrive(k):
        at = lax.rem(k, 9)
        sign = jnp.where(lax.rem(at, 2) == 1, SCALE, -SCALE)
        middle = jnp.logical_and(at > 2, at < 5)
        x = jnp.where(jnp.logical_or(at == 0, middle), 0.0, sign)
        y = jnp.where(at < 3, 0.0, jnp.where(at < 7, sign, -sign))
        z = code_offset(k // 9).astype(F32) * SCALE
        for d, moved in enumerate((x, y, z)):
            places[k, d : d + 1] = statics[k, d : d + 1] + moved

    for piece in fill(0, even, even_squares, even_damping):
        piece()
    geometry(0, even, even_squares, even_damping, even_weights, True)
    sums_a[...] = jnp.zeros_like(sums_a)

    def run_block(last, boxes):
        pending = functools.partial(charges, last, even_weights)
        held = (
            (odd, odd_squares, odd_damping, odd_weights),
            (even, even_squares, even_damping, even_weights),
        )
        for piece in fill(boxes[0], *held[0][:3]):
            piece()
        for at, k in enumerate(boxes):
            between = []
            if at + 1 < len(boxes):
                between = fill(boxes[at + 1], *held[(at + 1) % 2][:3])
            geometry(k, *held[at % 2], False, between + [pending])
            pending = functools.partial(charges, k, held[at % 2][3])

    near = jnp.where(lax.rem(mine[2], 4) == 3, 2, 1)
    far = 3 - near

    def enter(first, count, where):
        landed(statics.at[pl.ds(first, count)], static_recv.at[where])
        for at in range(count):
            arrive(jnp.int32(first + at))

    enter(1, 2, 0)
    run_block(0, [1, 2])
    enter(3, 2, 1)
    enter(5, 4, 2)
    run_block(2, [3, 4, 5, 6, 7, 8])
    enter(9 * near, 1, 3 * near)
    enter(9 * far, 1, 3 * far)
    run_block(8, [9 * near, 9 * far])

    def side_boxes(turn, last):
        side = jnp.where(turn == 0, near, far)
        enter(9 * side + 1, 4, 3 * side + 1)
        run_block(last, [9 * side + at for at in range(1, 5)])
        enter(9 * side + 5, 4, 3 * side + 2)
        run_block(9 * side + 4, [9 * side + at for at in range(5, 9)])
        return 9 * side + 8

    last = lax.fori_loop(0, 2, side_boxes, 9 * far)
    charges(last, even_weights)
    tall = sums_a[...]
    tall = tall[0:16] + tall[16:32] + tall[32:48]
    permanent = [place[d] * tall[0:1] - tall[1 + d : 2 + d] for d in range(3)]
    to_shift = jnp.where(live, DRUDE_GAIN * drude, 0.0)
    to_moment = to_shift * drude * (1.0 / CUTOFF**3)

    def induced(turn, boxes, first, corners=()):
        part_a = part_b = None
        for k in list(boxes) + list(corners):
            fine = k in boxes if isinstance(k, int) else any(k is box for box in boxes)
            mu = [moments[turn, k, d] for d in range(3)]
            at = [places[k, d : d + 1] for d in range(3)]
            along = at[0] * mu[0] + at[1] * mu[1] + at[2] * mu[2]
            rows = mu + [along]
            rows += [mu[d] * at[e] for e in range(3) for d in range(3)]
            rows += [along * at[e] for e in range(3)]
            high, rest = split(jnp.concatenate(rows, axis=0))
            middle, rest = split(rest)
            left = jnp.concatenate([high, middle, rest.astype(BF16)], axis=0)

            def through(coef, part, k=k, left=left, fine=fine):
                high, low = split(coef[k].reshape(SLOTS, SLOTS))
                for right in (high, low.astype(BF16)) if fine else (high,):
                    term = jnp.dot(left, right, preferred_element_type=F32)
                    part = term if part is None else part + term
                return part

            part_a = through(coef_a, part_a)
            part_b = through(coef_b, part_b)
        if first:
            sums_a[...] = part_a
            sums_b[...] = part_b
        else:
            sums_a[...] += part_a
            sums_b[...] += part_b

    def choose():
        lane1 = lax.broadcasted_iota(jnp.int32, (1, 128), 1)
        lane = lax.broadcasted_iota(jnp.int32, (MOVE, 128), 1)
        pick = lax.rem(lane, MOVE) == lax.broadcasted_iota(jnp.int32, (MOVE, 128), 0)
        pick = jnp.where(pick, 1.0, 0.0)
        flat = jnp.full((1, 128), -1.0, F32)
        for at in range(6):
            tiled = jnp.dot(
                jnp.broadcast_to(leaving_ref[at].astype(F32), (8, MOVE)),
                pick,
                precision=HIGHEST,
                preferred_element_type=F32,
            )[0:1]
            flat = jnp.where(lane1 // MOVE == at, tiled, flat)
        slot_rows = lax.broadcasted_iota(jnp.int32, (SLOTS, 128), 0).astype(F32)
        chosen[...] = jnp.where(slot_rows == flat, 1.0, 0.0).astype(BF16)
        listed[...] = jnp.broadcast_to(flat, (8, 128))

    for d in range(3):
        latest[3 + d : 4 + d] = permanent[d]
        latest[6 + d : 7 + d] = permanent[d]

    def turn_body(turn, carry):
        for d in range(3):
            field = latest[3 + d : 4 + d]
            latest[d : d + 1] = field
            moments[turn, 0, d] = to_moment * field
        for k in [1, 2] + list(range(26, 2, -1)):
            moment_copy(turn, mirror[k], peers[k]).start()
        induced(turn, [0], True)

        @pl.when(turn == 0)
        def _():
            choose()

        landed(moments.at[turn, pl.ds(1, 2)], moment_recv.at[turn, 0])
        induced(turn, [1, 2], False)
        landed(moments.at[turn, pl.ds(3, 2)], moment_recv.at[turn, 1])
        induced(turn, [3, 4], False)
        landed(moments.at[turn, pl.ds(5, 4)], moment_recv.at[turn, 2])
        landed(moments.at[turn, pl.ds(near * 9, 1)], moment_recv.at[turn, 3 * near])
        induced(turn, [5, 6, 7, 8, near * 9], False)
        landed(moments.at[turn, pl.ds(near * 9 + 1, 4)], moment_recv.at[turn, 3 * near + 1])
        landed(moments.at[turn, pl.ds(near * 9 + 5, 4)], moment_recv.at[turn, 3 * near + 2])
        near_corners = [near * 9 + at for at in range(5, 9)]
        induced(turn, [near * 9 + at for at in range(1, 5)], False, near_corners)
        landed(moments.at[turn, pl.ds(far * 9, 1)], moment_recv.at[turn, 3 * far])
        landed(moments.at[turn, pl.ds(far * 9 + 1, 4)], moment_recv.at[turn, 3 * far + 1])
        induced(turn, [far * 9 + at for at in range(5)], False)
        landed(moments.at[turn, pl.ds(far * 9 + 5, 4)], moment_recv.at[turn, 3 * far + 2])
        induced(turn, [], False, [far * 9 + at for at in range(5, 9)])
        landed(moments.at[turn, pl.ds(1, 26)], moment_send.at[turn])
        tall, wide = sums_a[...], sums_b[...]
        tall = tall[0:16] + tall[16:32] + tall[32:48]
        wide = wide[0:16] + wide[16:32] + wide[32:48]
        plain = place[0] * tall[0:1] + place[1] * tall[1:2] + place[2] * tall[2:3] - tall[3:4]
        for e in range(3):
            mixed = [place[d] * tall[4 + 3 * e + d : 5 + 3 * e + d] for d in range(3)]
            dipolar = place[e] * plain - (mixed[0] + mixed[1] + mixed[2]) + tall[13 + e : 14 + e]
            latest[3 + e : 4 + e] = latest[6 + e : 7 + e] + 3.0 * dipolar - wide[e : e + 1]
        return carry

    lax.fori_loop(0, ITERS, turn_body, 0)
    before = [latest[d : d + 1] for d in range(3)]
    fields = [latest[3 + d : 4 + d] for d in range(3)]
    shifts = [to_shift * before[d] for d in range(3)]

    mass = masses_ref[0]
    velocity = [velocity_ref[d] + KICK * charge * fields[d] / mass for d in range(3)]
    moved = [fractions[d] + (TIMESTEP / EDGE) * velocity[d] for d in range(3)]
    rows = moved + velocity + shifts
    rest = [charge, drude, screening, label, mass, jnp.zeros((2, SLOTS), F32)]
    complete = jnp.concatenate(rows + rest, axis=0)
    matches = chosen[...]
    flat = listed[0:1]
    high, rest = split(complete)
    middle, rest = split(rest)
    left = jnp.concatenate([high, middle, rest.astype(BF16)], axis=0)
    packed = jnp.dot(left, matches, preferred_element_type=F32)
    packed = packed[0:16] + packed[16:32] + packed[32:48]
    present = jnp.where(flat >= 0.0, 1.0, 0.0)
    face = lax.broadcasted_iota(jnp.int32, (1, 128), 1) // MOVE
    headings = []
    for d in range(3):
        heading = jnp.where(face == 2 * d, -1.0, 0.0) + jnp.where(face == 2 * d + 1, 1.0, 0.0)
        headings.append(heading * present)
    headings.append(jnp.zeros((13, 128), F32))
    outbox[...] = packed + jnp.concatenate(headings, axis=0)

    def out_copy(face, device):
        return pltpu.make_async_remote_copy(
            src_ref=outbox,
            dst_ref=inbox.at[face],
            send_sem=out_send,
            recv_sem=out_recv,
            device_id=device,
            device_id_type=MESH,
        )

    for at in range(5, -1, -1):
        out_copy(at, step_from(mine, sizes, UNITS[at])).start()
    named = lax.dot_general(
        jnp.ones((16, 128), BF16), matches, (((1,), (1,)), ((), ())), preferred_element_type=F32
    )[0:1]
    remain = jnp.logical_and(live, named < 0.5)
    for at in range(9):
        staying_ref[at] = jnp.where(remain, rows[at], 0.0)
    landed(statics.at[pl.ds(1, 26)], static_send)
    landed(inbox, out_recv)
    result = jnp.zeros((16, 128), F32)
    lane16 = lax.broadcasted_iota(jnp.int32, (16, 128), 1) // MOVE
    for at in range(6):
        result = jnp.where(lane16 == at, inbox[at], result)
    for at in range(14):
        arrivals_ref[at] = result[at : at + 1, 0 : 6 * MOVE]
    landed(inbox, out_send)


def solution(mesh):
    sizes = tuple(mesh.shape[axis] for axis in AXES)
    vec = P("gx", "gy", "gz", None, None)
    row = P("gx", "gy", "gz", None)
    placed = (vec, vec, row, row, row, row, row, P("gx", "gy", "gz"), vec)
    vmem = pl.BlockSpec(memory_space=pltpu.VMEM)
    hbm = pl.BlockSpec(memory_space=pltpu.HBM)
    call = pl.pallas_call(
        functools.partial(kernel, sizes),
        out_shape=(
            jax.ShapeDtypeStruct((9, 1, SLOTS), F32),
            jax.ShapeDtypeStruct((14, 1, 6 * MOVE), F32),
        ),
        in_specs=[hbm] * 7 + [pl.BlockSpec(memory_space=pl.ANY), hbm],
        out_specs=(vmem, vmem),
        scratch_shapes=[
            pltpu.VMEM((3, 1, SLOTS), F32),
            pltpu.VMEM((3, 1, SLOTS), F32),
            pltpu.VMEM((1, 1, SLOTS), F32),
            pltpu.VMEM((1, 1, SLOTS), F32),
            pltpu.VMEM((1, 1, SLOTS), F32),
            pltpu.VMEM((1, 1, SLOTS), jnp.int32),
            pltpu.VMEM((1, 1, SLOTS), F32),
            pltpu.VMEM((1, 1, 1), jnp.int32),
            pltpu.VMEM((6, 1, MOVE), jnp.int32),
            pltpu.VMEM((27, 8, SLOTS), F32),
            pltpu.VMEM((27, 4, SLOTS), F32),
            pltpu.VMEM((ITERS, 27, 3, 1, SLOTS), F32),
            pltpu.VMEM((GROUPS, 8, 128), F32),
            pltpu.VMEM((GROUPS, 8, 128), F32),
            pltpu.VMEM((GROUPS, 8, SLOTS), F32),
            pltpu.VMEM((GROUPS, 8, SLOTS), F32),
            pltpu.VMEM((GROUPS, 8, SLOTS), F32),
            pltpu.VMEM((GROUPS, 8, SLOTS), F32),
            pltpu.VMEM((2, SLOTS, SLOTS), BF16),
            pltpu.VMEM((2, SLOTS, SLOTS), BF16),
            pltpu.VMEM((27, GROUPS, 8, SLOTS), F32),
            pltpu.VMEM((27, GROUPS, 8, SLOTS), F32),
            pltpu.VMEM((48, SLOTS), F32),
            pltpu.VMEM((48, SLOTS), F32),
            pltpu.VMEM((SLOTS, 128), BF16),
            pltpu.VMEM((8, 128), F32),
            pltpu.VMEM((16, SLOTS), F32),
            pltpu.VMEM((16, 128), F32),
            pltpu.VMEM((6, 16, 128), F32),
            pltpu.SemaphoreType.DMA((9,)),
            pltpu.SemaphoreType.DMA,
            pltpu.SemaphoreType.DMA((9,)),
            pltpu.SemaphoreType.DMA((ITERS,)),
            pltpu.SemaphoreType.DMA((ITERS, 9)),
            pltpu.SemaphoreType.DMA,
            pltpu.SemaphoreType.DMA,
        ],
        compiler_params=pltpu.CompilerParams(
            collective_id=0, has_side_effects=True, vmem_limit_bytes=48 * 1024 * 1024
        ),
    )

    def local(fractions, velocity, charge, drude_charge, screening, labels, masses, counts, leaving):
        flat = [value.reshape(1, 1, SLOTS) for value in (charge, drude_charge, screening, labels, masses)]
        operands = [fractions.reshape(3, 1, SLOTS), velocity.reshape(3, 1, SLOTS), *flat, counts]
        operands.append(leaving.reshape(6, 1, MOVE))
        operands = [value if value.size == 1 else pltpu.with_memory_space_constraint(value, pltpu.HBM) for value in operands]
        staying, arrivals = call(*operands)
        return staying.reshape(1, 1, 1, 9, SLOTS), arrivals.reshape(1, 1, 1, 14, 6 * MOVE)

    return jax.shard_map(local, mesh=mesh, in_specs=placed, out_specs=(vec, vec), check_vma=False)
```
